32 devices in a mesh: tab: 8 (over z, x), rep: 4 (over y, core).
Axes of the slice: x: 2, y: 2, z: 4, core: 2. Of those that a mesh axis runs over, the one named last changes fastest.
Arguments:
- sample_ids: int32 [16384, 26], P(('tab', 'rep')), may hold values from 0 to 4095, as said below
- features: bfloat16 [16384, 27, 128], P(('tab', 'rep')), may hold values from -6 to 6
- pair_grad: bfloat16 [351, 16384], P(None, ('tab', 'rep')), may hold values from -1.59375 to 1.59375
Outputs:
- table_grad: float32 [26, 4096, 128], P(None, ('tab', 'rep'))
- dense_grad: float32 [16384, 128], P(('tab', 'rep'))
The draws below stay inside these ranges and needn't reach their ends.
Inputs may be any that keep to these rules, and one draw needn't show every extreme that they name: `sample_ids`: row r is owned by device r // 128, numbered tab * 4 + rep. For each field and the 512 samples of one device (aligned blocks of rows in device order), at most 32 ids fall in the rows of any one device, and at most 128 in the rows of any one tab index; in every block and field both bounds are reached.
All inputs are finite; a program needn't handle non-finite values.
Results may differ from the reference program's by a relative error of at most 0.0029.
Values may be sent and summed in bfloat16 or wider, within the bound.
No kernel may reach another device: no remote copies, remote signals or barrier semaphores. Data moves between devices by JAX's collectives and lax.ppermute only.
A program may use at most 128 MiB of HBM per device.

```python
import math
import jax
import jax.numpy as jnp
import numpy as np
from jax import lax

E = 128
F = 26
B_DEV = 512
RQ = 128
PAIRS = 351
BATCH = 16384
ROWS = 4096
CAP = 32
N_TAB = 8
N_REP = 4


def draw_sample_ids(key, part):
    blocks = N_TAB * N_REP
    key_hot = jax.random.fold_in(key, 11)
    key_pick = jax.random.fold_in(key, 12)
    key_mix = jax.random.fold_in(key, 13)
    key_rows = jax.random.fold_in(key, 14)
    hot_col = jax.random.randint(key_hot, (blocks * F, 1), 0, N_TAB)
    others = (blocks - N_REP) * CAP
    picks = jax.vmap(lambda k: jax.random.permutation(k, others))(jax.random.split(key_pick, blocks * F))
    chosen = picks[:, :B_DEV - N_REP * CAP] // CAP
    cold_owner = chosen + jnp.where(chosen >= hot_col * N_REP, N_REP, 0)
    hot_owner = hot_col * N_REP + (jnp.arange(N_REP * CAP, dtype=jnp.int32) // CAP)[None, :]
    all_owner = jnp.concatenate([hot_owner, cold_owner], axis=1)
    orders = jax.vmap(lambda k: jax.random.permutation(k, B_DEV))(jax.random.split(key_mix, blocks * F))
    all_owner = jnp.take_along_axis(all_owner, orders, axis=1)
    within = jax.random.randint(key_rows, all_owner.shape, 0, RQ)
    result = (all_owner * RQ + within).astype(jnp.int32)
    return result.reshape(blocks, F, B_DEV).transpose(0, 2, 1).reshape(blocks * B_DEV, F)


def steps_of(own_key, dims, pieces, smallest, top_value):
    def one(axis_at, parts):
        heights = jax.random.uniform(jax.random.fold_in(jax.random.fold_in(own_key, 6), axis_at), (parts,), jnp.float32, smallest / len(pieces), top_value / len(pieces))
        return jnp.repeat(jnp.exp(heights), dims[axis_at] // parts).reshape((-1,) + (1,) * (len(dims) - axis_at - 1))

    loudness = one(*pieces[0])
    for cut in pieces[1:]:
        loudness = loudness * one(*cut)
    return loudness


def noise(own_key, shape, width, limit, shards=(), held_as=jnp.bfloat16):
    level = steps_of(own_key, shape, shards, -0.22, 0.18) if shards else 1.0
    entries = jax.random.normal(own_key, shape, jnp.float32) * width * level
    return jnp.minimum(jnp.maximum(entries, -limit), limit).astype(held_as)


def setup_inputs(seed: int = 0) -> dict:
    key_list = jax.random.split(jax.random.key(seed), 4)
    sample_ids = draw_sample_ids(jax.random.fold_in(key_list[3], 71), 0)
    features = noise(key_list[1], (BATCH, F + 1, E), 1.0, 6.0, ((0, 32),))
    pair_grad = noise(key_list[2], (PAIRS, BATCH), 0.2, 1.59375, ((1, 32),))
    return {"sample_ids": sample_ids, "features": features, "pair_grad": pair_grad}


def pair_table(vectors):
    row_of, col_of = np.tril_indices(vectors, -1)
    spread = np.zeros((row_of.shape[0], vectors * vectors), np.float32)
    places = np.arange(row_of.shape[0])
    spread[places, row_of * vectors + col_of] = 1.0
    spread[places, col_of * vectors + row_of] = 1.0
    return spread


def reference(sample_ids, features, pair_grad):
    vectors = features.shape[1]
    spread = jnp.asarray(pair_table(vectors).T).astype(jnp.bfloat16)
    symmetric = jnp.dot(spread, pair_grad, preferred_element_type=jnp.float32)
    block_rows = math.gcd(BATCH, 4096)
    block_count = BATCH // block_rows

    def one_block(running, index):
        start = (index * block_rows).astype(jnp.int32)
        part_feat = lax.dynamic_slice_in_dim(features, start, block_rows, 0).astype(jnp.float32)
        part_sym = lax.dynamic_slice_in_dim(symmetric, start, block_rows, 1).reshape(vectors, vectors, block_rows)
        part_ids = lax.dynamic_slice_in_dim(sample_ids, start, block_rows, 0)
        gradients = jnp.einsum("fgb,bge->bfe", part_sym, part_feat)
        rounded = lax.optimization_barrier(gradients[:, 1:, :].astype(jnp.bfloat16)).astype(jnp.float32)
        fields_at = jnp.broadcast_to(jnp.arange(F, dtype=jnp.int32)[None, :], part_ids.shape)
        running = running.at[fields_at, part_ids].add(rounded)
        return running, gradients[:, 0, :]

    start_grad = jnp.zeros((F, ROWS, E), jnp.float32)
    table_grad, dense_parts = lax.scan(one_block, start_grad, jnp.arange(block_count, dtype=jnp.int32))
    return table_grad, dense_parts.reshape(BATCH, E)
```

```python
import functools
import math

import jax
import jax.numpy as jnp
import numpy as np
from jax import lax
from jax.experimental import pallas as pl
from jax.experimental.pallas import tpu as pltpu
from jax.sharding import PartitionSpec as P

RQ = 128
LANES = 128
PACK = 16
SUB = 8


def pair_spread(vectors, width):
    row_of, col_of = np.tril_indices(vectors, -1)
    spread = np.zeros((row_of.shape[0], vectors, SUB, width), np.float32)
    places = np.arange(row_of.shape[0])
    spread[places, row_of, :, col_of] = 1.0
    spread[places, col_of, :, row_of] = 1.0
    return spread.reshape(row_of.shape[0], -1)


def meta_kernel(fields, owners, window, ids_ref, earlier_ref, below_ref, rank_ref, meta_ref, mine, before):
    samples = ids_ref.shape[1]
    last_base = samples - window
    owner_at = lax.broadcasted_iota(jnp.int32, (owners, samples), 0)
    for field in range(fields):
        own = ids_ref[field : field + 1, :] // RQ
        mine[field * owners : (field + 1) * owners, :] = jnp.where(owner_at == own, 1.0, 0.0).astype(jnp.bfloat16)
    before[...] = jnp.dot(mine[...], earlier_ref[...], preferred_element_type=jnp.float32)
    slot_at = lax.broadcasted_iota(jnp.int32, (LANES, samples), 0).astype(jnp.float32)
    lane = lax.broadcasted_iota(jnp.int32, (owners, LANES), 1)
    for field in range(fields):
        rows = slice(field * owners, (field + 1) * owners)
        hit = mine[rows, :].astype(jnp.float32)
        count = jnp.sum(hit, axis=1, keepdims=True)
        count = jnp.broadcast_to(count, (owners, LANES)).astype(jnp.bfloat16)
        start = jnp.dot(below_ref[...], count, preferred_element_type=jnp.float32)
        tile = jnp.minimum(jnp.floor(start * (1.0 / PACK)), float(last_base // PACK))
        start, tile_of = start[:, :1], tile[:, :1]
        place = before[rows, :] + start
        rank = jnp.sum(hit * place, axis=0, keepdims=True)
        slot = jnp.sum(hit * (place - tile_of * PACK), axis=0, keepdims=True)
        rank_ref[field : field + 1, :] = rank
        tag = (ids_ref[field : field + 1, :] % RQ + 1).astype(jnp.float32)
        tags = lax.dot_general(
            (hit * tag).astype(jnp.bfloat16),
            jnp.where(slot_at == slot, 1.0, 0.0).astype(jnp.bfloat16),
            (((1,), (1,)), ((), ())),
            preferred_element_type=jnp.float32,
        )
        meta_ref[field] = jnp.where(lane == LANES - 1, tile, tags).astype(jnp.bfloat16)
    for field in range(fields, meta_ref.shape[0]):
        meta_ref[field] = jnp.zeros((owners, LANES), jnp.bfloat16)


def grads_kernel(fields, pairs_ref, spread_ref, feat_ref, rank_ref, dense_ref, sorted_ref, weights, grads):
    samples, vectors, depth = feat_ref.shape
    span = spread_ref.shape[1] // vectors
    width = span // SUB
    own_lane = (
        lax.broadcasted_iota(jnp.int32, (SUB, span), 1) // width == lax.broadcasted_iota(jnp.int32, (SUB, span), 0)
    )
    own_lane = jnp.concatenate([own_lane.astype(jnp.float32)] * (samples // SUB), axis=0)
    for vector in range(vectors):
        spread_out = jnp.dot(
            pairs_ref[...], spread_ref[:, vector * span : (vector + 1) * span], preferred_element_type=jnp.float32
        )
        weights[:, vector] = (spread_out * own_lane).reshape(samples // SUB, SUB, span)

    def per_group(group, carry):
        first = pl.multiple_of(group * SUB, SUB)
        block = feat_ref[pl.ds(first, SUB)]
        block = jnp.concatenate([block, jnp.zeros((SUB, width - vectors, depth), block.dtype)], axis=1)
        left = weights[group].reshape(vectors * SUB, span).astype(jnp.bfloat16)
        out = jnp.dot(left, block.reshape(span, depth), preferred_element_type=jnp.float32)
        out = out.reshape(vectors, SUB, depth)
        dense_ref[pl.ds(first, SUB), :] = out[0]
        grads[:, pl.ds(first, SUB), :] = out[1:]
        return carry

    lax.fori_loop(0, samples // SUB, per_group, 0, unroll=2)
    slot_at = lax.broadcasted_iota(jnp.int32, (samples, samples), 0).astype(jnp.float32)

    def per_field(field, carry):
        placing = jnp.where(slot_at == rank_ref[pl.ds(field, 1), :], 1.0, 0.0).astype(jnp.bfloat16)
        placed = jnp.dot(placing, grads[field].astype(jnp.bfloat16), preferred_element_type=jnp.float32)
        sorted_ref[field] = placed.astype(jnp.bfloat16)
        return carry

    lax.fori_loop(0, fields, per_field, 0)


def tally_kernel(window, tile_ref, tags_ref, data_ref, out_ref):
    _, blocks, samples, depth = data_ref.shape
    owners = tags_ref.shape[1]
    field = pl.program_id(0)
    row_at = (lax.broadcasted_iota(jnp.int32, (RQ, blocks * window), 0) + 1).astype(jnp.float32)

    def per_owner(owner, carry):
        parts = []
        for block in range(blocks):
            tile = tile_ref[(field * owners + owner) * blocks + block]
            parts.append(data_ref[0, block, pl.ds(pl.multiple_of(tile * PACK, PACK), window), :])
        matches = jnp.where(row_at == tags_ref[0, pl.ds(owner, 1), :], 1.0, 0.0).astype(jnp.bfloat16)
        summed = jnp.dot(matches, jnp.concatenate(parts, axis=0), preferred_element_type=jnp.float32)
        out_ref[owner, 0] = summed.astype(jnp.bfloat16)
        return carry

    lax.fori_loop(0, owners, per_owner, 0, unroll=2)


def local(outer, inner, sample_ids, features, pair_grad):
    samples, vectors, depth = features.shape
    fields = vectors - 1
    owners = outer * inner
    capacity = 2 * samples // owners
    window = min(-(-(PACK - 1 + capacity) // PACK) * PACK, samples)
    per_device = -(-fields // inner)
    width = 2 * LANES // SUB
    vmem = pl.BlockSpec(memory_space=pltpu.VMEM)
    params = pltpu.CompilerParams(vmem_limit_bytes=60 * 2**20)

    order = np.arange(samples)
    earlier = jnp.asarray(order[:, None] < order[None, :]).astype(jnp.bfloat16)
    below = jnp.asarray(np.arange(owners)[:, None] > np.arange(owners)[None, :]).astype(jnp.bfloat16)
    rank, meta = pl.pallas_call(
        functools.partial(meta_kernel, fields, owners, window),
        out_shape=(
            jax.ShapeDtypeStruct((fields, samples), jnp.float32),
            jax.ShapeDtypeStruct((per_device * inner, owners, LANES), jnp.bfloat16),
        ),
        in_specs=[vmem] * 3,
        out_specs=[vmem] * 2,
        scratch_shapes=[
            pltpu.VMEM((fields * owners, samples), jnp.bfloat16),
            pltpu.VMEM((fields * owners, samples), jnp.float32),
        ],
        compiler_params=params,
        name="meta",
    )(sample_ids.T, earlier, below)
    every = ("tab", "rep")
    groups = [list(range(first, first + inner)) for first in range(0, owners, inner)]
    exchange = functools.partial(
        lax.all_to_all, axis_name=every, split_axis=1, concat_axis=1, tiled=True, axis_index_groups=groups
    )
    meta = exchange(meta.reshape(per_device, inner, owners, LANES))
    tiles = meta[..., LANES - 1].astype(jnp.int32).transpose(0, 2, 1).reshape(-1)
    tags = meta[..., :window].transpose(0, 2, 1, 3).reshape(per_device, owners, inner * window).astype(jnp.float32)

    spread = jnp.asarray(pair_spread(vectors, width)).astype(jnp.bfloat16)
    dense_grad, in_order = pl.pallas_call(
        functools.partial(grads_kernel, fields),
        out_shape=(
            jax.ShapeDtypeStruct((samples, depth), jnp.float32),
            jax.ShapeDtypeStruct((per_device * inner, samples, depth), jnp.bfloat16),
        ),
        in_specs=[vmem] * 4,
        out_specs=[vmem] * 2,
        scratch_shapes=[
            pltpu.VMEM((samples // SUB, vectors, SUB, SUB * width), jnp.float32),
            pltpu.VMEM((fields, samples, depth), jnp.float32),
        ],
        compiler_params=params,
        name="grads",
    )(pair_grad.T, spread, features, rank)
    arrived = exchange(in_order.reshape(per_device, inner, samples, depth))
    partial_rows = pl.pallas_call(
        functools.partial(tally_kernel, window),
        out_shape=jax.ShapeDtypeStruct((owners, per_device, RQ, depth), jnp.bfloat16),
        grid_spec=pltpu.PrefetchScalarGridSpec(
            num_scalar_prefetch=1,
            grid=(per_device,),
            in_specs=[
                pl.BlockSpec((1, owners, inner * window), lambda f, _: (f, 0, 0)),
                pl.BlockSpec((1, inner, samples, depth), lambda f, _: (f, 0, 0, 0)),
            ],
            out_specs=pl.BlockSpec((owners, 1, RQ, depth), lambda f, _: (0, f, 0, 0)),
        ),
        compiler_params=params,
        name="tally",
    )(tiles, tags, arrived)
    rows = lax.all_to_all(partial_rows, every, split_axis=0, concat_axis=0, tiled=True)
    rows = rows.reshape(outer, inner, per_device, RQ, depth).astype(jnp.float32).sum(axis=0)
    table_grad = rows.transpose(1, 0, 2, 3).reshape(per_device * inner, RQ, depth)[:fields]
    return table_grad, dense_grad


def solution(mesh):
    tab, rep = mesh.shape["tab"], mesh.shape["rep"]
    inner = rep * math.gcd(tab, 4)
    every = ("tab", "rep")
    return jax.shard_map(
        functools.partial(local, tab * rep // inner, inner),
        mesh=mesh,
        in_specs=(P(every, None), P(every, None, None), P(None, every)),
        out_specs=(P(None, every, None), P(every, None)),
        check_vma=False,
    )
```

```python
import functools
import math

import jax
import jax.numpy as jnp
from jax import lax
from jax.experimental import pallas as pl
from jax.experimental.pallas import tpu as pltpu
from jax.sharding import PartitionSpec as P

RQ = 128
LANES = 128
PACK = 16
SUB = 8
HALVES = 2


def iota(shape, dim):
    return lax.broadcasted_iota(jnp.int32, shape, dim)


def one_hot(hit):
    return jnp.where(hit, 1.0, 0.0).astype(jnp.bfloat16)


def order_fields(first, count, owners, window, ids_ref, payload_ref, rank_ref, mine):
    samples = ids_ref.shape[1]
    pitch = LANES // HALVES
    last_tile = (samples - window) // PACK
    for at in range(count):
        own = ids_ref[first + at : first + at + 1, :] // RQ
        mine[at * owners : (at + 1) * owners, :] = one_hot(iota((owners, samples), 0) == own)
    earlier = one_hot(iota((samples, samples), 0) < iota((samples, samples), 1))
    before = jnp.dot(mine[...], earlier, preferred_element_type=jnp.float32)
    held = jnp.dot(mine[...], jnp.ones((samples, LANES), jnp.bfloat16), preferred_element_type=jnp.float32)
    below = one_hot(iota((owners, owners), 0) > iota((owners, owners), 1))
    slot_at = iota((LANES, samples), 0).astype(jnp.float32)
    lane = iota((owners // HALVES, LANES), 1)
    for at in range(count):
        rows = slice(at * owners, (at + 1) * owners)
        start = jnp.dot(below, held[rows].astype(jnp.bfloat16), preferred_element_type=jnp.float32)
        tile = jnp.minimum(jnp.floor(start * (1.0 / PACK)), float(last_tile))
        hit = mine[rows, :].astype(jnp.float32)
        place = hit * (before[rows] + jnp.concatenate([start] * (samples // LANES), axis=1))
        base = hit * jnp.concatenate([tile * PACK] * (samples // LANES), axis=1)
        rank = jnp.sum(place, axis=0, keepdims=True)
        slot = rank - jnp.sum(base, axis=0, keepdims=True)
        rank_ref[at : at + 1, :] = rank
        tag = (ids_ref[first + at : first + at + 1, :] % RQ + 1).astype(jnp.float32)
        tags = lax.dot_general(
            (hit * tag).astype(jnp.bfloat16),
            one_hot(slot_at == slot),
            (((1,), (1,)), ((), ())),
            preferred_element_type=jnp.float32,
        )
        half = owners // HALVES
        row = tags[:half] + pltpu.roll(tags[half:], pitch, 1)
        row = jnp.where(lane == pitch - 1, tile[:half], jnp.where(lane == LANES - 1, tile[half:], row))
        payload_ref[at, samples:, :] = row.astype(jnp.bfloat16)


def send_kernel(first, count, dense, owners, window, ids_ref, pairs_ref, feat_ref, *rest):
    if dense:
        dense_ref, payload_ref, rank_ref, mine, weights, grads = rest
    else:
        payload_ref, rank_ref, mine, weights, grads = rest
    vectors, samples, depth = feat_ref.shape
    span = 2 * LANES
    order_fields(first, count, owners, window, ids_ref, payload_ref, rank_ref, mine)
    for at in range(count, payload_ref.shape[0]):
        payload_ref[at] = jnp.zeros(payload_ref.shape[1:], jnp.bfloat16)

    targets = ([0] if dense else []) + list(range(first + 1, first + 1 + count))
    pairs = pairs_ref[...].astype(jnp.float32).T.astype(jnp.bfloat16)
    pair_at = iota((pairs.shape[1], span), 0)
    source = iota((1, span), 1) // SUB
    own_lane = one_hot(iota((PACK, span), 1) % SUB == iota((PACK, span), 0) % SUB)

    def spread_of(target):
        pair = jnp.where(source < target, target * (target - 1) // 2 + source, source * (source - 1) // 2 + target)
        pair = jnp.where((source == target) | (source >= vectors), -1, pair)
        found = jnp.dot(pairs, one_hot(pair_at == pair), preferred_element_type=jnp.float32)
        return found.reshape(samples // SUB, SUB, span)

    for at in range(0, len(targets), 2):
        low = spread_of(targets[at])
        high = spread_of(targets[at + 1]) if at + 1 < len(targets) else jnp.zeros_like(low)
        weights[:, at // 2] = jnp.concatenate([low, high], axis=1).astype(jnp.bfloat16) * own_lane

    def per_group(group, carry):
        begin = pl.multiple_of(group * PACK, PACK)
        block = feat_ref[:, pl.ds(begin, PACK), :].astype(jnp.float32)
        outs = []
        for part in range(PACK // SUB):
            right = block[:, part * SUB : (part + 1) * SUB, :].reshape(vectors * SUB, depth)
            right = jnp.concatenate([right, jnp.zeros((span - vectors * SUB, depth), jnp.float32)], axis=0)
            left = weights[group * (PACK // SUB) + part].reshape(-1, span)
            out = jnp.dot(left, right.astype(jnp.bfloat16), preferred_element_type=jnp.float32)
            outs.append(out.reshape(-1, SUB, depth))
        out = jnp.concatenate(outs, axis=1)
        if dense:
            dense_ref[pl.ds(begin, PACK), :] = out[0]
            out = out[1:]
        grads[:, pl.ds(begin, PACK), :] = out[:count].astype(jnp.bfloat16)
        return carry

    lax.fori_loop(0, samples // PACK, per_group, 0, unroll=2)
    slot_at = iota((samples, samples), 0).astype(jnp.float32)

    def per_field(at, carry):
        placing = one_hot(slot_at == rank_ref[pl.ds(at, 1), :])
        placed = jnp.dot(placing, grads[at], preferred_element_type=jnp.float32)
        payload_ref[at, :samples, :] = placed.astype(jnp.bfloat16)
        return carry

    lax.fori_loop(0, count, per_field, 0, unroll=2)


def tally_kernel(window, samples, data_ref, out_ref, tags, tiles, tile_at, done):
    blocks = data_ref.shape[0]
    owners = out_ref.shape[0]
    half, pitch = owners // HALVES, LANES // HALVES
    lane = iota((half, LANES), 1)
    tags[...] = jnp.zeros_like(tags)
    found = jnp.zeros((half, LANES), jnp.float32)
    for block in range(blocks):
        rows = data_ref[block, samples:, :].astype(jnp.float32)
        column, offset = divmod(block * window, LANES)
        for part in range(HALVES):
            own = slice(part * half, (part + 1) * half)
            tile_lane = part * blocks + block
            found = jnp.where(
                lane == tile_lane, pltpu.roll(rows, (tile_lane - (part * pitch + pitch - 1)) % LANES, 1), found
            )
            shifted = pltpu.roll(rows, (offset - part * pitch) % LANES, 1) if offset != part * pitch else rows
            fits = min(window, LANES - offset)
            here = slice(column * LANES, (column + 1) * LANES)
            tags[own, here] = jnp.where((lane >= offset) & (lane < offset + fits), shifted, tags[own, here])
            if fits < window:
                after = slice((column + 1) * LANES, (column + 2) * LANES)
                tags[own, after] = jnp.where(lane < window - fits, shifted, tags[own, after])
    tiles[...] = found.astype(jnp.int32)
    copy = pltpu.make_async_copy(tiles, tile_at, done)
    copy.start()
    copy.wait()
    row_at = (iota((RQ, blocks * window), 0) + 1).astype(jnp.float32)

    def per_owner(owner, carry):
        part, row = owner // half, owner % half
        picked = []
        for block in range(blocks):
            tile = tile_at[row, part * blocks + block]
            picked.append(data_ref[block, pl.ds(pl.multiple_of(tile * PACK, PACK), window), :])
        matches = one_hot(row_at == tags[pl.ds(owner, 1), : blocks * window])
        summed = jnp.dot(matches, jnp.concatenate(picked, axis=0), preferred_element_type=jnp.float32)
        out_ref[owner] = summed.astype(jnp.bfloat16)
        return carry

    lax.fori_loop(0, owners, per_owner, 0, unroll=4)


def local(outer, inner, sample_ids, features, pair_grad):
    samples, vectors, depth = features.shape
    fields = vectors - 1
    owners = outer * inner
    capacity = 2 * samples // owners
    window = min(-(-(PACK - 1 + capacity) // PACK) * PACK, samples)
    extra = owners // HALVES
    every = ("tab", "rep")
    groups = [list(range(start, start + inner)) for start in range(0, owners, inner)]
    vmem = pl.BlockSpec(memory_space=pltpu.VMEM)
    params = pltpu.CompilerParams(vmem_limit_bytes=60 * 2**20)
    ids = sample_ids.T
    by_vector = features.transpose(1, 0, 2)

    def send(first, count, dense):
        targets = count + dense
        shapes = [jax.ShapeDtypeStruct((inner, samples + extra, depth), jnp.bfloat16)]
        if dense:
            shapes = [jax.ShapeDtypeStruct((samples, depth), jnp.float32)] + shapes
        return pl.pallas_call(
            functools.partial(send_kernel, first, count, dense, owners, window),
            out_shape=shapes,
            in_specs=[vmem] * 3,
            out_specs=[vmem] * len(shapes),
            scratch_shapes=[
                pltpu.VMEM((count, samples), jnp.float32),
                pltpu.VMEM((count * owners, samples), jnp.bfloat16),
                pltpu.VMEM((samples // SUB, -(-targets // 2), PACK, 2 * LANES), jnp.bfloat16),
                pltpu.VMEM((count, samples, depth), jnp.bfloat16),
            ],
            cost_estimate=pl.CostEstimate(
                flops=2 * targets * samples * samples * depth, bytes_accessed=2 * features.size, transcendentals=0
            ),
            compiler_params=params,
            name="send",
        )(ids, pair_grad, by_vector)

    def tally(arrived):
        return pl.pallas_call(
            functools.partial(tally_kernel, window, samples),
            out_shape=jax.ShapeDtypeStruct((owners, RQ, depth), jnp.bfloat16),
            in_specs=[vmem],
            out_specs=vmem,
            scratch_shapes=[
                pltpu.VMEM((owners, -(-inner * window // LANES) * LANES), jnp.float32),
                pltpu.VMEM((extra, LANES), jnp.int32),
                pltpu.SMEM((extra, LANES), jnp.int32),
                pltpu.SemaphoreType.DMA,
            ],
            cost_estimate=pl.CostEstimate(
                flops=2 * owners * inner * window * RQ * depth, bytes_accessed=2 * arrived.size, transcendentals=0
            ),
            compiler_params=params,
            name="tally",
        )(arrived)

    firsts = list(range(0, fields, inner))
    outgoing = []
    for first in firsts:
        outgoing.append(send(first, min(inner, fields - first), first == firsts[-1]))
    dense_grad = outgoing[-1][0]
    tables = []
    for first, sent in zip(firsts, outgoing):
        arrived = lax.all_to_all(
            sent[-1], every, split_axis=0, concat_axis=0, tiled=True, axis_index_groups=groups
        )
        rows = lax.all_to_all(tally(arrived), every, split_axis=0, concat_axis=0, tiled=True)
        rows = rows.reshape(outer, inner, RQ, depth)[:, : min(inner, fields - first)]
        tables.append(rows.astype(jnp.float32).sum(axis=0))
    return jnp.concatenate(tables, axis=0), dense_grad


def solution(mesh):
    tab, rep = mesh.shape["tab"], mesh.shape["rep"]
    inner = rep * math.gcd(tab, 4)
    every = ("tab", "rep")
    return jax.shard_map(
        functools.partial(local, tab * rep // inner, inner),
        mesh=mesh,
        in_specs=(P(every, None), P(every, None, None), P(None, every)),
        out_specs=(P(None, every, None), P(every, None)),
        check_vma=False,
    )
```

```python
import functools
import math

import jax
import jax.numpy as jnp
from jax import lax
from jax.experimental import pallas as pl
from jax.experimental.pallas import tpu as pltpu
from jax.sharding import PartitionSpec as P

RQ = 128
LANES = 128
PACK = 16
SUB = 8
HALVES = 2


def iota(shape, dim):
    return lax.broadcasted_iota(jnp.int32, shape, dim)


def one_hot(hit):
    return jnp.where(hit, 1.0, 0.0).astype(jnp.bfloat16)


def order_fields(first, count, owners, window, ids_ref, payload_ref, rank_ref, mine):
    samples = ids_ref.shape[1]
    pitch = LANES // HALVES
    last_tile = (samples - window) // PACK
    for at in range(count):
        own = ids_ref[first + at : first + at + 1, :] // RQ
        mine[at * owners : (at + 1) * owners, :] = one_hot(iota((owners, samples), 0) == own)
    earlier = one_hot(iota((samples, samples), 0) < iota((samples, samples), 1))
    before = jnp.dot(mine[...], earlier, preferred_element_type=jnp.float32)
    held = jnp.dot(mine[...], jnp.ones((samples, LANES), jnp.bfloat16), preferred_element_type=jnp.float32)
    below = one_hot(iota((owners, owners), 0) > iota((owners, owners), 1))
    slot_at = iota((LANES, samples), 0).astype(jnp.float32)
    lane = iota((owners // HALVES, LANES), 1)
    for at in range(count):
        rows = slice(at * owners, (at + 1) * owners)
        start = jnp.dot(below, held[rows].astype(jnp.bfloat16), preferred_element_type=jnp.float32)
        tile = jnp.minimum(jnp.floor(start * (1.0 / PACK)), float(last_tile))
        hit = mine[rows, :].astype(jnp.float32)
        place = hit * (before[rows] + jnp.concatenate([start] * (samples // LANES), axis=1))
        base = hit * jnp.concatenate([tile * PACK] * (samples // LANES), axis=1)
        rank = jnp.sum(place, axis=0, keepdims=True)
        slot = rank - jnp.sum(base, axis=0, keepdims=True)
        rank_ref[at : at + 1, :] = rank
        tag = (ids_ref[first + at : first + at + 1, :] % RQ + 1).astype(jnp.float32)
        tags = lax.dot_general(
            (hit * tag).astype(jnp.bfloat16),
            one_hot(slot_at == slot),
            (((1,), (1,)), ((), ())),
            preferred_element_type=jnp.float32,
        )
        half = owners // HALVES
        row = tags[:half] + pltpu.roll(tags[half:], pitch, 1)
        row = jnp.where(lane == pitch - 1, tile[:half], jnp.where(lane == LANES - 1, tile[half:], row))
        payload_ref[at, samples:, :] = row.astype(jnp.bfloat16)


def send_kernel(first, count, dense, owners, window, ids_ref, pairs_ref, feat_ref, *rest):
    if dense:
        dense_ref, payload_ref, rank_ref, mine, weights, grads = rest
    else:
        payload_ref, rank_ref, mine, weights, grads = rest
    vectors, samples, depth = feat_ref.shape
    span = 2 * LANES
    order_fields(first, count, owners, window, ids_ref, payload_ref, rank_ref, mine)
    for at in range(count, payload_ref.shape[0]):
        payload_ref[at] = jnp.zeros(payload_ref.shape[1:], jnp.bfloat16)

    targets = ([0] if dense else []) + list(range(first + 1, first + 1 + count))
    pairs = pairs_ref[...].astype(jnp.float32).T.astype(jnp.bfloat16)
    pair_at = iota((pairs.shape[1], span), 0)
    source = iota((1, span), 1) // SUB
    own_lane = one_hot(iota((PACK, span), 1) % SUB == iota((PACK, span), 0) % SUB)

    def spread_of(target):
        pair = jnp.where(source < target, target * (target - 1) // 2 + source, source * (source - 1) // 2 + target)
        pair = jnp.where((source == target) | (source >= vectors), -1, pair)
        found = jnp.dot(pairs, one_hot(pair_at == pair), preferred_element_type=jnp.float32)
        return found.reshape(samples // SUB, SUB, span)

    for at in range(0, len(targets), 2):
        low = spread_of(targets[at])
        high = spread_of(targets[at + 1]) if at + 1 < len(targets) else jnp.zeros_like(low)
        weights[:, at // 2] = jnp.concatenate([low, high], axis=1).astype(jnp.bfloat16) * own_lane

    def per_group(group, carry):
        begin = pl.multiple_of(group * PACK, PACK)
        block = feat_ref[:, pl.ds(begin, PACK), :].astype(jnp.float32)
        outs = []
        for part in range(PACK // SUB):
            right = block[:, part * SUB : (part + 1) * SUB, :].reshape(vectors * SUB, depth)
            right = jnp.concatenate([right, jnp.zeros((span - vectors * SUB, depth), jnp.float32)], axis=0)
            left = weights[group * (PACK // SUB) + part].reshape(-1, span)
            out = jnp.dot(left, right.astype(jnp.bfloat16), preferred_element_type=jnp.float32)
            outs.append(out.reshape(-1, SUB, depth))
        out = jnp.concatenate(outs, axis=1)
        if dense:
            dense_ref[pl.ds(begin, PACK), :] = out[0]
            out = out[1:]
        grads[:, pl.ds(begin, PACK), :] = out[:count].astype(jnp.bfloat16)
        return carry

    lax.fori_loop(0, samples // PACK, per_group, 0, unroll=2)
    slot_at = iota((samples, samples), 0).astype(jnp.float32)

    def per_field(at, carry):
        placing = one_hot(slot_at == rank_ref[pl.ds(at, 1), :])
        placed = jnp.dot(placing, grads[at], preferred_element_type=jnp.float32)
        payload_ref[at, :samples, :] = placed.astype(jnp.bfloat16)
        return carry

    lax.fori_loop(0, count, per_field, 0, unroll=2)


def tally_kernel(window, samples, near, first_ref, data_ref, *rest):
    if near:
        near_ref, out_ref, tags, tiles, tile_at, done = rest
    else:
        out_ref, tags, tiles, tile_at, done = rest
    blocks = data_ref.shape[0]
    owners = out_ref.shape[0] + near
    half, pitch = owners // HALVES, LANES // HALVES
    lane = iota((half, LANES), 1)
    tags[...] = jnp.zeros_like(tags)
    found = jnp.zeros((half, LANES), jnp.float32)
    for block in range(blocks):
        rows = data_ref[block, samples:, :].astype(jnp.float32)
        column, offset = divmod(block * window, LANES)
        for part in range(HALVES):
            own = slice(part * half, (part + 1) * half)
            tile_lane = part * blocks + block
            found = jnp.where(
                lane == tile_lane, pltpu.roll(rows, (tile_lane - (part * pitch + pitch - 1)) % LANES, 1), found
            )
            shifted = pltpu.roll(rows, (offset - part * pitch) % LANES, 1) if offset != part * pitch else rows
            fits = min(window, LANES - offset)
            here = slice(column * LANES, (column + 1) * LANES)
            tags[own, here] = jnp.where((lane >= offset) & (lane < offset + fits), shifted, tags[own, here])
            if fits < window:
                after = slice((column + 1) * LANES, (column + 2) * LANES)
                tags[own, after] = jnp.where(lane < window - fits, shifted, tags[own, after])
    tiles[...] = found.astype(jnp.int32)
    copy = pltpu.make_async_copy(tiles, tile_at, done)
    copy.start()
    copy.wait()
    row_at = (iota((RQ, blocks * window), 0) + 1).astype(jnp.float32)

    def rows_of(owner):
        part, row = owner // half, owner % half
        picked = []
        for block in range(blocks):
            tile = tile_at[row, part * blocks + block]
            picked.append(data_ref[block, pl.ds(pl.multiple_of(tile * PACK, PACK), window), :])
        matches = one_hot(row_at == tags[pl.ds(owner, 1), : blocks * window])
        return jnp.dot(matches, jnp.concatenate(picked, axis=0), preferred_element_type=jnp.float32)

    def per_near(at, carry):
        near_ref[at] = rows_of((first_ref[0] + at) % owners)
        return carry

    def per_far(at, carry):
        out_ref[at] = rows_of((first_ref[0] + near + at) % owners).astype(jnp.bfloat16)
        return carry

    if near:
        lax.fori_loop(0, near, per_near, 0, unroll=4)
    lax.fori_loop(0, owners - near, per_far, 0, unroll=4)


def local(outer, inner, sample_ids, features, pair_grad):
    samples, vectors, depth = features.shape
    fields = vectors - 1
    owners = outer * inner
    capacity = 2 * samples // owners
    window = min(-(-(PACK - 1 + capacity) // PACK) * PACK, samples)
    extra = owners // HALVES
    every = ("tab", "rep")
    groups = [list(range(start, start + inner)) for start in range(0, owners, inner)]
    vmem = pl.BlockSpec(memory_space=pltpu.VMEM)
    params = pltpu.CompilerParams(vmem_limit_bytes=40 * 2**20)
    ids = sample_ids.T
    by_vector = features.transpose(1, 0, 2)

    def send(first, count, dense):
        targets = count + dense
        shapes = [jax.ShapeDtypeStruct((inner, samples + extra, depth), jnp.bfloat16)]
        if dense:
            shapes = [jax.ShapeDtypeStruct((samples, depth), jnp.float32)] + shapes
        return pl.pallas_call(
            functools.partial(send_kernel, first, count, dense, owners, window),
            out_shape=shapes,
            in_specs=[vmem] * 3,
            out_specs=[vmem] * len(shapes),
            scratch_shapes=[
                pltpu.VMEM((count, samples), jnp.float32),
                pltpu.VMEM((count * owners, samples), jnp.bfloat16),
                pltpu.VMEM((samples // SUB, -(-targets // 2), PACK, 2 * LANES), jnp.bfloat16),
                pltpu.VMEM((count, samples, depth), jnp.bfloat16),
            ],
            cost_estimate=pl.CostEstimate(
                flops=2 * targets * samples * samples * depth, bytes_accessed=2 * features.size, transcendentals=0
            ),
            compiler_params=params,
            name="send",
        )(ids, pair_grad, by_vector)

    def tally(arrived, first, near):
        shapes = [jax.ShapeDtypeStruct((owners - near, RQ, depth), jnp.bfloat16)]
        if near:
            shapes = [jax.ShapeDtypeStruct((near, RQ, depth), jnp.float32)] + shapes
        return pl.pallas_call(
            functools.partial(tally_kernel, window, samples, near),
            out_shape=shapes,
            in_specs=[pl.BlockSpec(memory_space=pltpu.SMEM), vmem],
            out_specs=[vmem] * len(shapes),
            scratch_shapes=[
                pltpu.VMEM((owners, -(-inner * window // LANES) * LANES), jnp.float32),
                pltpu.VMEM((extra, LANES), jnp.int32),
                pltpu.SMEM((extra, LANES), jnp.int32),
                pltpu.SemaphoreType.DMA,
            ],
            cost_estimate=pl.CostEstimate(
                flops=2 * owners * inner * window * RQ * depth, bytes_accessed=2 * arrived.size, transcendentals=0
            ),
            compiler_params=pltpu.CompilerParams(vmem_limit_bytes=24 * 2**20),
            name="tally",
        )(jnp.reshape(first, (1,)).astype(jnp.int32), arrived)

    def exchange(blocks, groups):
        return lax.all_to_all(blocks, every, split_axis=0, concat_axis=0, tiled=True, axis_index_groups=groups)

    def relayed(sent):
        mine, others = tally(exchange(sent, groups), lax.axis_index(every) // inner * inner, inner)
        others = others.reshape(outer - 1, inner, RQ, depth)
        total = mine
        for hop in range(1, outer):
            total += lax.ppermute(
                others[hop - 1], every, [(at, (at + hop * inner) % owners) for at in range(owners)]
            ).astype(jnp.float32)
        return exchange(total.astype(jnp.bfloat16), groups).astype(jnp.float32)

    def direct(sent):
        (rows,) = tally(exchange(sent, groups), jnp.int32(0), 0)
        return exchange(rows, None).reshape(outer, inner, RQ, depth).astype(jnp.float32).sum(axis=0)

    tail = fields - fields % inner
    dense_grad, sent = send(tail, fields - tail, True)
    last = relayed(sent)[: fields - tail]
    tables = [direct(send(first, inner, False)[0]) for first in range(0, tail, inner)]
    return jnp.concatenate(tables + [last], axis=0), dense_grad


def solution(mesh):
    tab, rep = mesh.shape["tab"], mesh.shape["rep"]
    inner = rep * math.gcd(tab, 4)
    every = ("tab", "rep")
    return jax.shard_map(
        functools.partial(local, tab * rep // inner, inner),
        mesh=mesh,
        in_specs=(P(every, None), P(every, None, None), P(None, every)),
        out_specs=(P(None, every, None), P(every, None)),
        check_vma=False,
    )
```

```python
import functools
import math

import jax
import jax.numpy as jnp
from jax import lax
from jax.experimental import pallas as pl
from jax.experimental.pallas import tpu as pltpu
from jax.sharding import PartitionSpec as P

RQ = 128
LANES = 128
PACK = 16
SUB = 8
HALVES = 2
PARTS = 4
GROUP = LANES // PARTS


def iota(shape, dim):
    return lax.broadcasted_iota(jnp.int32, shape, dim)


def one_hot(hit):
    return jnp.where(hit, 1.0, 0.0).astype(jnp.bfloat16)


def order_fields(first, count, owners, window, ids_ref, store, rank_ref, mine):
    samples = ids_ref.shape[1]
    pitch = LANES // HALVES
    last_tile = (samples - window) // PACK
    for at in range(count):
        own = ids_ref[first + at : first + at + 1, :] // RQ
        mine[at * owners : (at + 1) * owners, :] = one_hot(iota((owners, samples), 0) == own)
    earlier = one_hot(iota((samples, samples), 0) < iota((samples, samples), 1))
    before = jnp.dot(mine[...], earlier, preferred_element_type=jnp.float32)
    held = jnp.dot(mine[...], jnp.ones((samples, LANES), jnp.bfloat16), preferred_element_type=jnp.float32)
    below = one_hot(iota((owners, owners), 0) > iota((owners, owners), 1))
    slot_at = iota((LANES, samples), 0).astype(jnp.float32)
    lane = iota((owners // HALVES, LANES), 1)
    for at in range(count):
        rows = slice(at * owners, (at + 1) * owners)
        start = jnp.dot(below, held[rows].astype(jnp.bfloat16), preferred_element_type=jnp.float32)
        tile = jnp.minimum(jnp.floor(start * (1.0 / PACK)), float(last_tile))
        hit = mine[rows, :].astype(jnp.float32)
        place = hit * (before[rows] + jnp.concatenate([start] * (samples // LANES), axis=1))
        base = hit * jnp.concatenate([tile * PACK] * (samples // LANES), axis=1)
        rank = jnp.sum(place, axis=0, keepdims=True)
        slot = rank - jnp.sum(base, axis=0, keepdims=True)
        rank_ref[at : at + 1, :] = rank
        tag = (ids_ref[first + at : first + at + 1, :] % RQ + 1).astype(jnp.float32)
        tags = lax.dot_general(
            (hit * tag).astype(jnp.bfloat16),
            one_hot(slot_at == slot),
            (((1,), (1,)), ((), ())),
            preferred_element_type=jnp.float32,
        )
        half = owners // HALVES
        row = tags[:half] + pltpu.roll(tags[half:], pitch, 1)
        row = jnp.where(lane == pitch - 1, tile[:half], jnp.where(lane == LANES - 1, tile[half:], row))
        store(at, row.astype(jnp.bfloat16))


def fold(block):
    kept = block.shape[0] * (PARTS - 1) // PARTS
    moved = [pltpu.roll(block[kept:], (PARTS - 1 - part) * GROUP, 1) for part in range(PARTS - 1)]
    last_group = iota((kept, LANES), 1) >= LANES - GROUP
    return jnp.where(last_group, jnp.concatenate(moved, axis=0), block[:kept])


def unfold(block):
    rows = block.shape[0] // (PARTS - 1)
    group = iota((rows, LANES), 1) // GROUP
    parts = [pltpu.roll(block[part * rows : (part + 1) * rows], (part + 1) * GROUP, 1) for part in range(PARTS - 1)]
    return jnp.where(group == 0, parts[0], jnp.where(group == 1, parts[1], parts[2]))


def fold_last(blocks):
    rows = blocks[0].shape[0] // PARTS
    kept = rows * (PARTS - 1)
    group = iota((kept, LANES), 1) // GROUP
    out = jnp.zeros((kept, LANES), blocks[0].dtype)
    tails = [jnp.zeros((rows, LANES), blocks[0].dtype)] * (PARTS - 1)
    for part, block in enumerate(blocks):
        out = jnp.where(group == part, pltpu.roll(block[:kept], (part + 1) * GROUP, 1), out)
        tails[part] = block[kept:]
    return jnp.where(group == PARTS - 1, jnp.concatenate(tails, axis=0), out)


def send_kernel(first, count, tail, owners, window, ids_ref, pairs_ref, feat_ref, *rest):
    if tail:
        dense_ref, payload_ref, rank_ref, mine, weights, grads = rest
    else:
        payload_ref, rank_ref, mine, weights, grads = rest
    dense = tail
    vectors, samples, depth = feat_ref.shape
    span = 2 * LANES
    body = samples * (PARTS - 1) // PARTS if tail else samples
    extra = owners // HALVES
    whole = count + -(-count // 2) if tail else count
    for at in range(count, payload_ref.shape[0]):
        payload_ref[at, body:] = jnp.zeros((payload_ref.shape[1] - body, LANES), jnp.bfloat16)
    for at in range(whole, payload_ref.shape[0]):
        payload_ref[at, :body] = jnp.zeros((body, LANES), jnp.bfloat16)

    def store(at, row):
        payload_ref[at, body : body + extra, :] = row
        if tail:
            payload_ref[at, body + extra :, :] = row
            place = body + at % 2 * extra
            payload_ref[count + at // 2, place : place + extra, :] = row

    order_fields(first, count, owners, window, ids_ref, store, rank_ref, mine)
    targets = ([0] if dense else []) + list(range(first + 1, first + 1 + count))
    pairs = pairs_ref[...].astype(jnp.float32).T.astype(jnp.bfloat16)
    pair_at = iota((pairs.shape[1], span), 0)
    source = iota((1, span), 1) // SUB
    own_lane = one_hot(iota((PACK, span), 1) % SUB == iota((PACK, span), 0) % SUB)

    def spread_of(target):
        pair = jnp.where(source < target, target * (target - 1) // 2 + source, source * (source - 1) // 2 + target)
        pair = jnp.where((source == target) | (source >= vectors), -1, pair)
        found = jnp.dot(pairs, one_hot(pair_at == pair), preferred_element_type=jnp.float32)
        return found.reshape(samples // SUB, SUB, span)

    for at in range(0, len(targets), 2):
        low = spread_of(targets[at])
        high = spread_of(targets[at + 1]) if at + 1 < len(targets) else jnp.zeros_like(low)
        weights[:, at // 2] = jnp.concatenate([low, high], axis=1).astype(jnp.bfloat16) * own_lane

    def per_group(group, carry):
        begin = pl.multiple_of(group * PACK, PACK)
        block = feat_ref[:, pl.ds(begin, PACK), :].astype(jnp.float32)
        outs = []
        for part in range(PACK // SUB):
            right = block[:, part * SUB : (part + 1) * SUB, :].reshape(vectors * SUB, depth)
            right = jnp.concatenate([right, jnp.zeros((span - vectors * SUB, depth), jnp.float32)], axis=0)
            left = weights[group * (PACK // SUB) + part].reshape(-1, span)
            out = jnp.dot(left, right.astype(jnp.bfloat16), preferred_element_type=jnp.float32)
            outs.append(out.reshape(-1, SUB, depth))
        out = jnp.concatenate(outs, axis=1)
        if dense:
            dense_ref[pl.ds(begin, PACK), :] = out[0]
            out = out[1:]
        grads[:, pl.ds(begin, PACK), :] = out[:count].astype(jnp.bfloat16)
        return carry

    lax.fori_loop(0, samples // PACK, per_group, 0, unroll=2)
    slot_at = iota((samples, samples), 0).astype(jnp.float32)

    def placed(at):
        placing = one_hot(slot_at == rank_ref[pl.ds(at, 1), :])
        return jnp.dot(placing, grads[at], preferred_element_type=jnp.float32)

    if tail:
        for at in range(0, count, 2):
            blocks = [placed(each) for each in range(at, min(at + 2, count))]
            for each, block in enumerate(blocks):
                payload_ref[at + each, :body, :] = fold(block).astype(jnp.bfloat16)
            payload_ref[count + at // 2, :body, :] = fold_last(blocks).astype(jnp.bfloat16)
    else:

        def per_field(at, carry):
            payload_ref[at, :body, :] = placed(at).astype(jnp.bfloat16)
            return carry

        lax.fori_loop(0, count, per_field, 0, unroll=2)


def read_tags(window, blocks, first_row, data_ref, tags, tiles):
    half, pitch = tiles.shape[0], LANES // HALVES
    lane = iota((half, LANES), 1)
    tags[...] = jnp.zeros_like(tags)
    found = jnp.zeros((half, LANES), jnp.float32)
    for block in range(blocks):
        rows = data_ref[block, first_row : first_row + half, :].astype(jnp.float32)
        column, offset = divmod(block * window, LANES)
        for part in range(HALVES):
            own = slice(part * half, (part + 1) * half)
            tile_lane = part * blocks + block
            found = jnp.where(
                lane == tile_lane, pltpu.roll(rows, (tile_lane - (part * pitch + pitch - 1)) % LANES, 1), found
            )
            shifted = pltpu.roll(rows, (offset - part * pitch) % LANES, 1) if offset != part * pitch else rows
            fits = min(window, LANES - offset)
            here = slice(column * LANES, (column + 1) * LANES)
            tags[own, here] = jnp.where((lane >= offset) & (lane < offset + fits), shifted, tags[own, here])
            if fits < window:
                after = slice((column + 1) * LANES, (column + 2) * LANES)
                tags[own, after] = jnp.where(lane < window - fits, shifted, tags[own, after])
    tiles[...] = found.astype(jnp.int32)


def rows_of(window, owner, sorted_ref, tags, tile_at):
    blocks = sorted_ref.shape[0]
    half = tile_at.shape[0]
    part, row = owner // half, owner % half
    row_at = (iota((RQ, blocks * window), 0) + 1).astype(jnp.float32)
    picked = []
    for block in range(blocks):
        tile = tile_at[row, part * blocks + block]
        picked.append(sorted_ref[block, pl.ds(pl.multiple_of(tile * PACK, PACK), window), :])
    matches = one_hot(row_at == tags[pl.ds(owner, 1), : blocks * window])
    return jnp.dot(matches, jnp.concatenate(picked, axis=0), preferred_element_type=jnp.float32)


def tally_kernel(window, samples, data_ref, tail_ref, out_ref, tags, tiles, tile_at, done):
    read_tags(window, data_ref.shape[0], samples, data_ref, tags, tiles)
    copy = pltpu.make_async_copy(tiles, tile_at, done)
    copy.start()
    out_ref[:, RQ:, :] = tail_ref[...]
    copy.wait()

    def per_owner(owner, carry):
        out_ref[owner, :RQ, :] = rows_of(window, owner, data_ref, tags, tile_at).astype(jnp.bfloat16)
        return carry

    lax.fori_loop(0, out_ref.shape[0], per_owner, 0, unroll=4)


def tally_tail_kernel(window, samples, data_ref, out_ref, unfolded, tags, tags_b, tiles, tiles_b, tile_at, tile_at_b, done):
    blocks = data_ref.shape[0]
    body = samples * (PARTS - 1) // PARTS
    read_tags(window, blocks, body, data_ref, tags, tiles)
    read_tags(window, blocks, body + tiles.shape[0], data_ref, tags_b, tiles_b)
    copy = pltpu.make_async_copy(tiles, tile_at, done.at[0])
    copy_b = pltpu.make_async_copy(tiles_b, tile_at_b, done.at[1])
    copy.start()
    copy_b.start()
    for block in range(blocks):
        unfolded[block, :body, :] = data_ref[block, :body, :]
        unfolded[block, body:, :] = unfold(data_ref[block, :body, :].astype(jnp.float32)).astype(jnp.bfloat16)
    copy.wait()
    copy_b.wait()
    second = iota((RQ, LANES), 1) // GROUP == 1

    def per_owner(owner, carry):
        rows = rows_of(window, owner, unfolded, tags, tile_at)
        rows_b = rows_of(window, owner, unfolded, tags_b, tile_at_b)
        out_ref[owner] = fold(jnp.where(second, rows_b, rows)).astype(jnp.bfloat16)
        return carry

    lax.fori_loop(0, out_ref.shape[0], per_owner, 0, unroll=2)


def finish_kernel(count, data_ref, table_ref):
    inner = data_ref.shape[1]
    kept = RQ * (PARTS - 1) // PARTS
    rest = RQ - kept
    tails = []
    for at in range(inner):
        total = jnp.sum(data_ref[:, at].astype(jnp.float32), axis=0)
        table_ref[at] = total[:RQ]
        tails.append(total[RQ:])
    own = iota((RQ, LANES), 1) < LANES - GROUP
    for at in range(count):
        part, block, other = at % 2, tails[at], tails[count + at // 2]
        main = jnp.concatenate([block, unfold(block)], axis=0)
        last = pltpu.roll(other, (PARTS - 1 - part) * GROUP, 1)
        last = jnp.concatenate([last, other[part * rest : (part + 1) * rest]], axis=0)
        table_ref[inner + at] = jnp.where(own, main, last)


def local(outer, inner, sample_ids, features, pair_grad):
    samples, vectors, depth = features.shape
    fields = vectors - 1
    owners = outer * inner
    capacity = 2 * samples // owners
    window = min(-(-(PACK - 1 + capacity) // PACK) * PACK, samples)
    extra = owners // HALVES
    tail = fields - inner
    if depth != LANES or not 0 < tail + -(-tail // 2) <= inner:
        raise ValueError("unsupported sizes")
    every = ("tab", "rep")
    groups = [list(range(start, start + inner)) for start in range(0, owners, inner)]
    vmem = pl.BlockSpec(memory_space=pltpu.VMEM)
    params = pltpu.CompilerParams(vmem_limit_bytes=40 * 2**20)
    ids = sample_ids.T
    by_vector = features.transpose(1, 0, 2)
    tail_samples = samples * (PARTS - 1) // PARTS
    tail_rows = RQ * (PARTS - 1) // PARTS
    tag_shape = (owners, -(-inner * window // LANES) * LANES)

    def send(first, count, is_tail):
        targets = count + is_tail
        rows = tail_samples + 2 * extra if is_tail else samples + extra
        shapes = [jax.ShapeDtypeStruct((inner, rows, depth), jnp.bfloat16)]
        if is_tail:
            shapes = [jax.ShapeDtypeStruct((samples, depth), jnp.float32)] + shapes
        return pl.pallas_call(
            functools.partial(send_kernel, first, count, is_tail, owners, window),
            out_shape=shapes,
            in_specs=[vmem] * 3,
            out_specs=[vmem] * len(shapes),
            scratch_shapes=[
                pltpu.VMEM((count, samples), jnp.float32),
                pltpu.VMEM((count * owners, samples), jnp.bfloat16),
                pltpu.VMEM((samples // SUB, -(-targets // 2), PACK, 2 * LANES), jnp.bfloat16),
                pltpu.VMEM((count, samples, depth), jnp.bfloat16),
            ],
            cost_estimate=pl.CostEstimate(
                flops=2 * targets * samples * samples * depth, bytes_accessed=2 * features.size, transcendentals=0
            ),
            compiler_params=params,
            name="send",
        )(ids, pair_grad, by_vector)

    def exchange(blocks, groups):
        return lax.all_to_all(blocks, every, split_axis=0, concat_axis=0, tiled=True, axis_index_groups=groups)

    small = pltpu.CompilerParams(vmem_limit_bytes=28 * 2**20)
    cost = pl.CostEstimate(
        flops=2 * owners * inner * window * RQ * depth, bytes_accessed=4 * inner * samples * depth, transcendentals=0
    )
    dense_grad, sent_tail = send(inner, tail, True)
    arrived_tail = exchange(sent_tail, groups)
    rows_tail = pl.pallas_call(
        functools.partial(tally_tail_kernel, window, samples),
        out_shape=jax.ShapeDtypeStruct((owners, tail_rows, depth), jnp.bfloat16),
        in_specs=[vmem],
        out_specs=vmem,
        scratch_shapes=[
            pltpu.VMEM((inner, samples, depth), jnp.bfloat16),
            pltpu.VMEM(tag_shape, jnp.float32),
            pltpu.VMEM(tag_shape, jnp.float32),
            pltpu.VMEM((extra, LANES), jnp.int32),
            pltpu.VMEM((extra, LANES), jnp.int32),
            pltpu.SMEM((extra, LANES), jnp.int32),
            pltpu.SMEM((extra, LANES), jnp.int32),
            pltpu.SemaphoreType.DMA((2,)),
        ],
        cost_estimate=cost,
        compiler_params=small,
        name="tally_tail",
    )(arrived_tail)
    arrived = exchange(send(0, inner, False)[0], groups)
    rows = pl.pallas_call(
        functools.partial(tally_kernel, window, samples),
        out_shape=jax.ShapeDtypeStruct((owners, RQ + tail_rows, depth), jnp.bfloat16),
        in_specs=[vmem] * 2,
        out_specs=vmem,
        scratch_shapes=[
            pltpu.VMEM(tag_shape, jnp.float32),
            pltpu.VMEM((extra, LANES), jnp.int32),
            pltpu.SMEM((extra, LANES), jnp.int32),
            pltpu.SemaphoreType.DMA,
        ],
        cost_estimate=cost,
        compiler_params=small,
        name="tally",
    )(arrived, rows_tail)
    table_grad = pl.pallas_call(
        functools.partial(finish_kernel, tail),
        out_shape=jax.ShapeDtypeStruct((fields, RQ, depth), jnp.float32),
        in_specs=[vmem],
        out_specs=vmem,
        compiler_params=small,
        name="finish",
    )(exchange(rows, None).reshape(outer, inner, RQ + tail_rows, depth))
    return table_grad, dense_grad


def solution(mesh):
    tab, rep = mesh.shape["tab"], mesh.shape["rep"]
    inner = rep * math.gcd(tab, 4)
    every = ("tab", "rep")
    return jax.shard_map(
        functools.partial(local, tab * rep // inner, inner),
        mesh=mesh,
        in_specs=(P(every, None), P(every, None, None), P(None, every)),
        out_specs=(P(None, every, None), P(every, None)),
        check_vma=False,
    )
```

```python
import functools
import math

import jax
import jax.numpy as jnp
from jax import lax
from jax.experimental import pallas as pl
from jax.experimental.pallas import tpu as pltpu
from jax.sharding import PartitionSpec as P

RQ = 128
LANES = 128
PACK = 16
SUB = 8
HALVES = 2
PARTS = 4
GROUP = LANES // PARTS
GROUP_UNROLL = 8
EXACT = 256


def iota(shape, dim):
    return lax.broadcasted_iota(jnp.int32, shape, dim)


def one_hot(hit):
    return jnp.where(hit, 1.0, 0.0).astype(jnp.bfloat16)


def order_fields(first, count, owners, window, ids_ref, store, rank_ref, mine):
    samples = ids_ref.shape[1]
    pitch = LANES // HALVES
    last_tile = (samples - window) // PACK
    for at in range(count):
        own = ids_ref[first + at : first + at + 1, :] // RQ
        mine[at * owners : (at + 1) * owners, :] = one_hot(iota((owners, samples), 0) == own)
    earlier = one_hot(iota((samples, samples), 0) < iota((samples, samples), 1))
    before = jnp.dot(mine[...], earlier, preferred_element_type=jnp.float32)
    held = jnp.dot(mine[...], jnp.ones((samples, LANES), jnp.bfloat16), preferred_element_type=jnp.float32)
    below = one_hot(iota((owners, owners), 0) > iota((owners, owners), 1))
    slot_at = iota((LANES, samples), 0).astype(jnp.float32)
    lane = iota((owners // HALVES, LANES), 1)
    for at in range(count):
        rows = slice(at * owners, (at + 1) * owners)
        start = jnp.dot(below, held[rows].astype(jnp.bfloat16), preferred_element_type=jnp.float32)
        tile = jnp.minimum(jnp.floor(start * (1.0 / PACK)), float(last_tile))
        hit = mine[rows, :].astype(jnp.float32)
        place = hit * (before[rows] + jnp.concatenate([start] * (samples // LANES), axis=1))
        base = hit * jnp.concatenate([tile * PACK] * (samples // LANES), axis=1)
        rank = jnp.sum(place, axis=0, keepdims=True)
        slot = rank - jnp.sum(base, axis=0, keepdims=True)
        rank_ref[at : at + 1, :] = rank
        tag = (ids_ref[first + at : first + at + 1, :] % RQ + 1).astype(jnp.float32)
        tags = lax.dot_general(
            (hit * tag).astype(jnp.bfloat16),
            one_hot(slot_at == slot),
            (((1,), (1,)), ((), ())),
            preferred_element_type=jnp.float32,
        )
        half = owners // HALVES
        row = tags[:half] + pltpu.roll(tags[half:], pitch, 1)
        row = jnp.where(lane == pitch - 1, tile[:half], jnp.where(lane == LANES - 1, tile[half:], row))
        store(at, row.astype(jnp.bfloat16))


def fold(block):
    kept = block.shape[0] * (PARTS - 1) // PARTS
    moved = [pltpu.roll(block[kept:], (PARTS - 1 - part) * GROUP, 1) for part in range(PARTS - 1)]
    last_group = iota((kept, LANES), 1) >= LANES - GROUP
    return jnp.where(last_group, jnp.concatenate(moved, axis=0), block[:kept])


def unfold(block):
    rows = block.shape[0] // (PARTS - 1)
    group = iota((rows, LANES), 1) // GROUP
    parts = [pltpu.roll(block[part * rows : (part + 1) * rows], (part + 1) * GROUP, 1) for part in range(PARTS - 1)]
    return jnp.where(group == 0, parts[0], jnp.where(group == 1, parts[1], parts[2]))


def fold_last(blocks):
    rows = blocks[0].shape[0] // PARTS
    kept = rows * (PARTS - 1)
    group = iota((kept, LANES), 1) // GROUP
    out = jnp.zeros((kept, LANES), blocks[0].dtype)
    tails = [jnp.zeros((rows, LANES), blocks[0].dtype)] * (PARTS - 1)
    for part, block in enumerate(blocks):
        out = jnp.where(group == part, pltpu.roll(block[:kept], (part + 1) * GROUP, 1), out)
        tails[part] = block[kept:]
    return jnp.where(group == PARTS - 1, jnp.concatenate(tails, axis=0), out)


def send_kernel(first, count, tail, owners, window, ids_hbm, pairs_hbm, feat_hbm, *rest):
    if tail:
        payload_hbm, *rest = rest
    else:
        dense_ref, payload_hbm, *rest = rest
    ids_ref, pairs_ref, feat_ref, payload_ref, rank_ref, mine, weights, grads, in_done, out_done = rest
    inputs = [
        pltpu.make_async_copy(source, target, in_done.at[at])
        for at, (source, target) in enumerate([(ids_hbm, ids_ref), (pairs_hbm, pairs_ref), (feat_hbm, feat_ref)])
    ]
    for copy in inputs:
        copy.start()

    def leave(at):
        return pltpu.make_async_copy(payload_ref.at[at], payload_hbm.at[at], out_done.at[at])

    vectors, samples, depth = feat_ref.shape
    span = 2 * LANES
    body = samples * (PARTS - 1) // PARTS if tail else samples
    extra = owners // HALVES
    whole = count + -(-count // 2) if tail else count
    for at in range(count, payload_ref.shape[0]):
        payload_ref[at, body:] = jnp.zeros((payload_ref.shape[1] - body, LANES), jnp.bfloat16)
    for at in range(whole, payload_ref.shape[0]):
        payload_ref[at, :body] = jnp.zeros((body, LANES), jnp.bfloat16)
        leave(at).start()

    def store(at, row):
        payload_ref[at, body : body + extra, :] = row
        if tail:
            payload_ref[at, body + extra :, :] = row
            place = body + at % 2 * extra
            payload_ref[count + at // 2, place : place + extra, :] = row

    inputs[0].wait()
    order_fields(first, count, owners, window, ids_ref, store, rank_ref, mine)
    targets = ([] if tail else [0]) + list(range(first + 1, first + 1 + count))
    inputs[1].wait()
    pairs = pairs_ref[...].astype(jnp.float32).T.astype(jnp.bfloat16)
    pair_at = iota((pairs.shape[1], span), 0)
    source = iota((1, span), 1) // SUB
    own_lane = one_hot(iota((PACK, span), 1) % SUB == iota((PACK, span), 0) % SUB)

    def spread_of(target):
        pair = jnp.where(source < target, target * (target - 1) // 2 + source, source * (source - 1) // 2 + target)
        pair = jnp.where((source == target) | (source >= vectors), -1, pair)
        found = jnp.dot(pairs, one_hot(pair_at == pair), preferred_element_type=jnp.float32)
        return found.reshape(samples // SUB, SUB, span)

    for at in range(0, len(targets), 2):
        low = spread_of(targets[at])
        high = spread_of(targets[at + 1]) if at + 1 < len(targets) else jnp.zeros_like(low)
        weights[:, at // 2] = jnp.concatenate([low, high], axis=1).astype(jnp.bfloat16) * own_lane
    inputs[2].wait()

    def per_group(group, carry):
        begin = pl.multiple_of(group * PACK, PACK)
        block = feat_ref[:, pl.ds(begin, PACK), :].astype(jnp.float32)
        outs = []
        for part in range(PACK // SUB):
            right = block[:, part * SUB : (part + 1) * SUB, :].reshape(vectors * SUB, depth)
            right = jnp.concatenate([right, jnp.zeros((span - vectors * SUB, depth), jnp.float32)], axis=0)
            left = weights[group * (PACK // SUB) + part].reshape(-1, span)
            out = jnp.dot(left, right.astype(jnp.bfloat16), preferred_element_type=jnp.float32)
            outs.append(out.reshape(-1, SUB, depth))
        out = jnp.concatenate(outs, axis=1)
        if not tail:
            dense_ref[pl.ds(begin, PACK), :] = out[0]
            out = out[1:]
        grads[:, pl.ds(begin, PACK), :] = out[:count].astype(jnp.bfloat16)
        return carry

    lax.fori_loop(0, samples // PACK, per_group, 0, unroll=GROUP_UNROLL)
    near = math.gcd(samples, EXACT)
    slot_at = iota((near, samples), 0).astype(jnp.float32).astype(jnp.bfloat16)

    def placed(at):
        rank = rank_ref[pl.ds(at, 1), :]
        tiles = []
        for top in range(0, samples, near):
            here = jnp.broadcast_to((rank - top).astype(jnp.bfloat16), (near, samples))
            tiles.append(jnp.where(slot_at == here, jnp.bfloat16(1), jnp.bfloat16(0)))
        placing = jnp.concatenate(tiles, axis=0)
        return jnp.dot(placing, grads[at], preferred_element_type=jnp.float32)

    if tail:
        for at in range(0, count, 2):
            blocks = [placed(each) for each in range(at, min(at + 2, count))]
            for each, block in enumerate(blocks):
                payload_ref[at + each, :body, :] = fold(block).astype(jnp.bfloat16)
                leave(at + each).start()
            payload_ref[count + at // 2, :body, :] = fold_last(blocks).astype(jnp.bfloat16)
            leave(count + at // 2).start()
    else:

        def per_field(at, carry):
            payload_ref[at, :body, :] = placed(at).astype(jnp.bfloat16)
            leave(at).start()
            return carry

        lax.fori_loop(0, count, per_field, 0, unroll=2)
    for at in range(payload_ref.shape[0]):
        leave(at).wait()


def read_tags(window, blocks, first_row, data_ref, tags, tiles):
    half, pitch = tiles.shape[0], LANES // HALVES
    lane = iota((half, LANES), 1)
    tags[...] = jnp.zeros_like(tags)
    found = jnp.zeros((half, LANES), jnp.float32)
    for block in range(blocks):
        rows = data_ref[block, first_row : first_row + half, :].astype(jnp.float32)
        column, offset = divmod(block * window, LANES)
        for part in range(HALVES):
            own = slice(part * half, (part + 1) * half)
            tile_lane = part * blocks + block
            found = jnp.where(
                lane == tile_lane, pltpu.roll(rows, (tile_lane - (part * pitch + pitch - 1)) % LANES, 1), found
            )
            shifted = pltpu.roll(rows, (offset - part * pitch) % LANES, 1) if offset != part * pitch else rows
            fits = min(window, LANES - offset)
            here = slice(column * LANES, (column + 1) * LANES)
            tags[own, here] = jnp.where((lane >= offset) & (lane < offset + fits), shifted, tags[own, here])
            if fits < window:
                after = slice((column + 1) * LANES, (column + 2) * LANES)
                tags[own, after] = jnp.where(lane < window - fits, shifted, tags[own, after])
    tiles[...] = found.astype(jnp.int32)


def rows_of(window, owner, sorted_ref, tags, tile_at):
    blocks = sorted_ref.shape[0]
    half = tile_at.shape[0]
    part, row = owner // half, owner % half
    row_at = (iota((RQ, blocks * window), 0) + 1).astype(jnp.float32)
    picked = []
    for block in range(blocks):
        tile = tile_at[row, part * blocks + block]
        picked.append(sorted_ref[block, pl.ds(pl.multiple_of(tile * PACK, PACK), window), :])
    matches = one_hot(row_at == tags[pl.ds(owner, 1), : blocks * window])
    return jnp.dot(matches, jnp.concatenate(picked, axis=0), preferred_element_type=jnp.float32)


def tally_kernel(window, samples, data_ref, tail_ref, out_ref, tags, tiles, tile_at, done):
    read_tags(window, data_ref.shape[0], samples, data_ref, tags, tiles)
    copy = pltpu.make_async_copy(tiles, tile_at, done)
    copy.start()
    out_ref[:, RQ:, :] = tail_ref[...]
    copy.wait()

    def per_owner(owner, carry):
        out_ref[owner, :RQ, :] = rows_of(window, owner, data_ref, tags, tile_at).astype(jnp.bfloat16)
        return carry

    lax.fori_loop(0, out_ref.shape[0], per_owner, 0, unroll=4)


def tally_tail_kernel(window, samples, data_ref, out_ref, unfolded, tags, tags_b, tiles, tiles_b, tile_at, tile_at_b, done):
    blocks = data_ref.shape[0]
    body = samples * (PARTS - 1) // PARTS
    read_tags(window, blocks, body, data_ref, tags, tiles)
    read_tags(window, blocks, body + tiles.shape[0], data_ref, tags_b, tiles_b)
    copy = pltpu.make_async_copy(tiles, tile_at, done.at[0])
    copy_b = pltpu.make_async_copy(tiles_b, tile_at_b, done.at[1])
    copy.start()
    copy_b.start()
    for block in range(blocks):
        unfolded[block, :body, :] = data_ref[block, :body, :]
        unfolded[block, body:, :] = unfold(data_ref[block, :body, :].astype(jnp.float32)).astype(jnp.bfloat16)
    copy.wait()
    copy_b.wait()
    second = iota((RQ, LANES), 1) // GROUP == 1

    def per_owner(owner, carry):
        rows = rows_of(window, owner, unfolded, tags, tile_at)
        rows_b = rows_of(window, owner, unfolded, tags_b, tile_at_b)
        out_ref[owner] = fold(jnp.where(second, rows_b, rows)).astype(jnp.bfloat16)
        return carry

    lax.fori_loop(0, out_ref.shape[0], per_owner, 0, unroll=2)


def finish_kernel(count, data_ref, table_ref):
    inner = data_ref.shape[1]
    kept = RQ * (PARTS - 1) // PARTS
    rest = RQ - kept
    tails = []
    for at in range(inner):
        total = jnp.sum(data_ref[:, at].astype(jnp.float32), axis=0)
        table_ref[at] = total[:RQ]
        tails.append(total[RQ:])
    own = iota((RQ, LANES), 1) < LANES - GROUP
    for at in range(count):
        part, block, other = at % 2, tails[at], tails[count + at // 2]
        main = jnp.concatenate([block, unfold(block)], axis=0)
        last = pltpu.roll(other, (PARTS - 1 - part) * GROUP, 1)
        last = jnp.concatenate([last, other[part * rest : (part + 1) * rest]], axis=0)
        table_ref[inner + at] = jnp.where(own, main, last)


def local(outer, inner, sample_ids, features, pair_grad):
    samples, vectors, depth = features.shape
    fields = vectors - 1
    owners = outer * inner
    capacity = 2 * samples // owners
    window = min(-(-(PACK - 1 + capacity) // PACK) * PACK, samples)
    extra = owners // HALVES
    tail = fields - inner
    if depth != LANES or not 0 < tail + -(-tail // 2) <= inner:
        raise ValueError("unsupported sizes")
    every = ("tab", "rep")
    groups = [list(range(start, start + inner)) for start in range(0, owners, inner)]
    vmem = pl.BlockSpec(memory_space=pltpu.VMEM)
    params = pltpu.CompilerParams(vmem_limit_bytes=63 * 2**20)
    ids = sample_ids.T
    by_vector = features.transpose(1, 0, 2)
    tail_samples = samples * (PARTS - 1) // PARTS
    tail_rows = RQ * (PARTS - 1) // PARTS
    tag_shape = (owners, -(-inner * window // LANES) * LANES)

    def send(first, count, is_tail):
        targets = count + 1 - is_tail
        rows = tail_samples + 2 * extra if is_tail else samples + extra
        shapes = [jax.ShapeDtypeStruct((inner, rows, depth), jnp.bfloat16)]
        specs = [pl.BlockSpec(memory_space=pl.ANY)]
        if not is_tail:
            shapes = [jax.ShapeDtypeStruct((samples, depth), jnp.float32)] + shapes
            specs = [vmem] + specs
        return pl.pallas_call(
            functools.partial(send_kernel, first, count, is_tail, owners, window),
            out_shape=shapes,
            in_specs=[pl.BlockSpec(memory_space=pl.ANY)] * 3,
            out_specs=specs,
            scratch_shapes=[
                pltpu.VMEM(ids.shape, ids.dtype),
                pltpu.VMEM(pair_grad.shape, pair_grad.dtype),
                pltpu.VMEM(by_vector.shape, by_vector.dtype),
                pltpu.VMEM((inner, rows, depth), jnp.bfloat16),
                pltpu.VMEM((count, samples), jnp.float32),
                pltpu.VMEM((count * owners, samples), jnp.bfloat16),
                pltpu.VMEM((samples // SUB, -(-targets // 2), PACK, 2 * LANES), jnp.bfloat16),
                pltpu.VMEM((count, samples, depth), jnp.bfloat16),
                pltpu.SemaphoreType.DMA((3,)),
                pltpu.SemaphoreType.DMA((inner,)),
            ],
            cost_estimate=pl.CostEstimate(
                flops=2 * targets * samples * samples * depth, bytes_accessed=2 * features.size, transcendentals=0
            ),
            compiler_params=params,
            name="send",
        )(ids, pair_grad, by_vector)

    def exchange(blocks, groups):
        return lax.all_to_all(blocks, every, split_axis=0, concat_axis=0, tiled=True, axis_index_groups=groups)

    small = pltpu.CompilerParams(vmem_limit_bytes=28 * 2**20)
    cost = pl.CostEstimate(
        flops=2 * owners * inner * window * RQ * depth, bytes_accessed=4 * inner * samples * depth, transcendentals=0
    )
    arrived_tail = exchange(send(inner, tail, True)[0], groups)
    dense_grad, sent = send(0, inner, False)
    rows_tail = pl.pallas_call(
        functools.partial(tally_tail_kernel, window, samples),
        out_shape=jax.ShapeDtypeStruct((owners, tail_rows, depth), jnp.bfloat16),
        in_specs=[vmem],
        out_specs=vmem,
        scratch_shapes=[
            pltpu.VMEM((inner, samples, depth), jnp.bfloat16),
            pltpu.VMEM(tag_shape, jnp.float32),
            pltpu.VMEM(tag_shape, jnp.float32),
            pltpu.VMEM((extra, LANES), jnp.int32),
            pltpu.VMEM((extra, LANES), jnp.int32),
            pltpu.SMEM((extra, LANES), jnp.int32),
            pltpu.SMEM((extra, LANES), jnp.int32),
            pltpu.SemaphoreType.DMA((2,)),
        ],
        cost_estimate=cost,
        compiler_params=small,
        name="tally_tail",
    )(arrived_tail)
    arrived = exchange(sent, groups)
    rows = pl.pallas_call(
        functools.partial(tally_kernel, window, samples),
        out_shape=jax.ShapeDtypeStruct((owners, RQ + tail_rows, depth), jnp.bfloat16),
        in_specs=[vmem] * 2,
        out_specs=vmem,
        scratch_shapes=[
            pltpu.VMEM(tag_shape, jnp.float32),
            pltpu.VMEM((extra, LANES), jnp.int32),
            pltpu.SMEM((extra, LANES), jnp.int32),
            pltpu.SemaphoreType.DMA,
        ],
        cost_estimate=cost,
        compiler_params=small,
        name="tally",
    )(arrived, rows_tail)
    table_grad = pl.pallas_call(
        functools.partial(finish_kernel, tail),
        out_shape=jax.ShapeDtypeStruct((fields, RQ, depth), jnp.float32),
        in_specs=[vmem],
        out_specs=vmem,
        compiler_params=small,
        name="finish",
    )(exchange(rows, None).reshape(outer, inner, RQ + tail_rows, depth))
    return table_grad, dense_grad


def solution(mesh):
    tab, rep = mesh.shape["tab"], mesh.shape["rep"]
    inner = rep * math.gcd(tab, 4)
    every = ("tab", "rep")
    return jax.shard_map(
        functools.partial(local, tab * rep // inner, inner),
        mesh=mesh,
        in_specs=(P(every, None), P(every, None, None), P(None, every)),
        out_specs=(P(None, every, None), P(every, None)),
        check_vma=False,
    )
```

```python
import functools
import math

import jax
import jax.numpy as jnp
from jax import lax
from jax.experimental import pallas as pl
from jax.experimental.pallas import tpu as pltpu
from jax.sharding import PartitionSpec as P

RQ = 128
LANES = 128
PACK = 16
SUB = 8
HALVES = 2
PARTS = 8
GROUP = LANES // PARTS
GROUP_UNROLL = 8
EXACT = 256


def iota(shape, dim):
    return lax.broadcasted_iota(jnp.int32, shape, dim)


def one_hot(hit):
    return jnp.where(hit, 1.0, 0.0).astype(jnp.bfloat16)


def order_fields(first, count, owners, window, ids_ref, store, rank_ref, mine):
    samples = ids_ref.shape[1]
    pitch = LANES // HALVES
    last_tile = (samples - window) // PACK
    for at in range(count):
        own = ids_ref[first + at : first + at + 1, :] // RQ
        mine[at * owners : (at + 1) * owners, :] = one_hot(iota((owners, samples), 0) == own)
    earlier = one_hot(iota((samples, samples), 0) < iota((samples, samples), 1))
    before = jnp.dot(mine[...], earlier, preferred_element_type=jnp.float32)
    held = jnp.dot(mine[...], jnp.ones((samples, LANES), jnp.bfloat16), preferred_element_type=jnp.float32)
    below = one_hot(iota((owners, owners), 0) > iota((owners, owners), 1))
    slot_at = iota((LANES, samples), 0).astype(jnp.float32)
    lane = iota((owners // HALVES, LANES), 1)
    for at in range(count):
        rows = slice(at * owners, (at + 1) * owners)
        start = jnp.dot(below, held[rows].astype(jnp.bfloat16), preferred_element_type=jnp.float32)
        tile = jnp.minimum(jnp.floor(start * (1.0 / PACK)), float(last_tile))
        hit = mine[rows, :].astype(jnp.float32)
        place = hit * (before[rows] + jnp.concatenate([start] * (samples // LANES), axis=1))
        base = hit * jnp.concatenate([tile * PACK] * (samples // LANES), axis=1)
        rank = jnp.sum(place, axis=0, keepdims=True)
        slot = rank - jnp.sum(base, axis=0, keepdims=True)
        rank_ref[at : at + 1, :] = rank
        tag = (ids_ref[first + at : first + at + 1, :] % RQ + 1).astype(jnp.float32)
        tags = lax.dot_general(
            (hit * tag).astype(jnp.bfloat16),
            one_hot(slot_at == slot),
            (((1,), (1,)), ((), ())),
            preferred_element_type=jnp.float32,
        )
        half = owners // HALVES
        row = tags[:half] + pltpu.roll(tags[half:], pitch, 1)
        row = jnp.where(lane == pitch - 1, tile[:half], jnp.where(lane == LANES - 1, tile[half:], row))
        store(at, row.astype(jnp.bfloat16))


def lane_group(rows):
    return iota((rows, LANES), 1) // GROUP


def shift(block, groups):
    return pltpu.roll(block, groups * GROUP % LANES, 1) if groups % PARTS else block


def pick(block, first, count, other):
    group = lane_group(block.shape[0])
    return jnp.where((group >= first) & (group < first + count), block, other)


def fold(block, keep):
    rows = block.shape[0] // PARTS
    out = []
    for part in range(keep):
        kept = block[part * rows : (part + 1) * rows]
        for at in range(keep, PARTS):
            kept = pick(shift(block[at * rows : (at + 1) * rows], at - part), at, 1, kept)
        out.append(kept)
    return jnp.concatenate(out, axis=0)


def unfold(block, keep):
    rows = block.shape[0] // keep
    out = []
    for at in range(keep, PARTS):
        moved = jnp.zeros((rows, LANES), block.dtype)
        for part in range(keep):
            moved = pick(shift(block[part * rows : (part + 1) * rows], part - at), part, 1, moved)
        out.append(moved)
    return jnp.concatenate(out, axis=0)


def share_out(count, devices):
    keep = -(-count * PARTS // devices)
    rest, others = PARTS - keep, devices - count
    singles = keep - rest
    if singles < 0 or (count - others) * rest > others * singles:
        raise ValueError("unsupported sizes")
    pieces = [(at, 0, at, keep, 0, rest) for at in range(min(others, count))]
    for at in range(max(count - others, 0) * rest):
        slot = at % singles
        pieces.append((at // singles, 1 + slot, others + at // rest, keep + at % rest, rest + slot, 1))
    return keep, 1 + singles, pieces


def send_kernel(first, count, tail, owners, window, ids_hbm, pairs_hbm, feat_hbm, *rest):
    if tail:
        payload_hbm, *rest = rest
    else:
        dense_ref, payload_hbm, *rest = rest
    ids_ref, pairs_ref, feat_ref, payload_ref, rank_ref, mine, weights, grads, in_done, out_done = rest
    inputs = [
        pltpu.make_async_copy(source, target, in_done.at[at])
        for at, (source, target) in enumerate([(ids_hbm, ids_ref), (pairs_hbm, pairs_ref), (feat_hbm, feat_ref)])
    ]
    for copy in inputs:
        copy.start()

    def leave(at):
        return pltpu.make_async_copy(payload_ref.at[at], payload_hbm.at[at], out_done.at[at])

    vectors, samples, depth = feat_ref.shape
    span = 2 * LANES
    keep, slots, pieces = share_out(count, payload_ref.shape[0]) if tail else (PARTS, 1, [])
    body = samples * keep // PARTS
    extra = owners // HALVES
    for at in range(count, payload_ref.shape[0]):
        payload_ref[at, body:] = jnp.zeros((payload_ref.shape[1] - body, LANES), jnp.bfloat16)

    def store(at, row):
        homes = [(at, slot) for slot in range(slots)]
        homes += [(count + device, slot) for device, slot, field, *_ in pieces if field == at]
        for device, slot in homes:
            payload_ref[device, body + slot * extra : body + (slot + 1) * extra, :] = row

    inputs[0].wait()
    order_fields(first, count, owners, window, ids_ref, store, rank_ref, mine)
    targets = ([] if tail else [0]) + list(range(first + 1, first + 1 + count))
    inputs[1].wait()
    pairs = pairs_ref[...].astype(jnp.float32).T.astype(jnp.bfloat16)
    pair_at = iota((pairs.shape[1], span), 0)
    source = iota((1, span), 1) // SUB
    own_lane = one_hot(iota((PACK, span), 1) % SUB == iota((PACK, span), 0) % SUB)

    def spread_of(target):
        pair = jnp.where(source < target, target * (target - 1) // 2 + source, source * (source - 1) // 2 + target)
        pair = jnp.where((source == target) | (source >= vectors), -1, pair)
        found = jnp.dot(pairs, one_hot(pair_at == pair), preferred_element_type=jnp.float32)
        return found.reshape(samples // SUB, SUB, span)

    for at in range(0, len(targets), 2):
        low = spread_of(targets[at])
        high = spread_of(targets[at + 1]) if at + 1 < len(targets) else jnp.zeros_like(low)
        weights[:, at // 2] = jnp.concatenate([low, high], axis=1).astype(jnp.bfloat16) * own_lane
    inputs[2].wait()

    def per_group(group, carry):
        begin = pl.multiple_of(group * PACK, PACK)
        block = feat_ref[:, pl.ds(begin, PACK), :].astype(jnp.float32)
        outs = []
        for part in range(PACK // SUB):
            right = block[:, part * SUB : (part + 1) * SUB, :].reshape(vectors * SUB, depth)
            right = jnp.concatenate([right, jnp.zeros((span - vectors * SUB, depth), jnp.float32)], axis=0)
            left = weights[group * (PACK // SUB) + part].reshape(-1, span)
            out = jnp.dot(left, right.astype(jnp.bfloat16), preferred_element_type=jnp.float32)
            outs.append(out.reshape(-1, SUB, depth))
        out = jnp.concatenate(outs, axis=1)
        if not tail:
            dense_ref[pl.ds(begin, PACK), :] = out[0]
            out = out[1:]
        grads[:, pl.ds(begin, PACK), :] = out[:count].astype(jnp.bfloat16)
        return carry

    lax.fori_loop(0, samples // PACK, per_group, 0, unroll=GROUP_UNROLL)
    near = math.gcd(samples, EXACT)
    slot_at = iota((near, samples), 0).astype(jnp.float32).astype(jnp.bfloat16)

    def placed(at):
        rank = rank_ref[pl.ds(at, 1), :]
        tiles = []
        for top in range(0, samples, near):
            here = jnp.broadcast_to((rank - top).astype(jnp.bfloat16), (near, samples))
            tiles.append(jnp.where(slot_at == here, jnp.bfloat16(1), jnp.bfloat16(0)))
        placing = jnp.concatenate(tiles, axis=0)
        return jnp.dot(placing, grads[at], preferred_element_type=jnp.float32)

    if tail:
        for at in range(count):
            block = placed(at)
            grads[at] = block.astype(jnp.bfloat16)
            payload_ref[at, :body, :] = fold(block, keep).astype(jnp.bfloat16)
            leave(at).start()
        for at in range(payload_ref.shape[0] - count):
            block = jnp.zeros((samples, LANES), jnp.float32)
            for device, _, field, source, target, groups in pieces:
                if device == at:
                    block = pick(shift(grads[field].astype(jnp.float32), target - source), target, groups, block)
            payload_ref[count + at, :body, :] = fold(block, keep).astype(jnp.bfloat16)
            leave(count + at).start()
    else:

        def per_field(at, carry):
            payload_ref[at, :body, :] = placed(at).astype(jnp.bfloat16)
            leave(at).start()
            return carry

        lax.fori_loop(0, count, per_field, 0, unroll=2)
    for at in range(payload_ref.shape[0]):
        leave(at).wait()


def read_tags(window, blocks, first_row, data_ref, tags, tiles):
    half, pitch = tiles.shape[0], LANES // HALVES
    lane = iota((half, LANES), 1)
    tags[...] = jnp.zeros_like(tags)
    found = jnp.zeros((half, LANES), jnp.float32)
    for block in range(blocks):
        rows = data_ref[block, first_row : first_row + half, :].astype(jnp.float32)
        column, offset = divmod(block * window, LANES)
        for part in range(HALVES):
            own = slice(part * half, (part + 1) * half)
            tile_lane = part * blocks + block
            found = jnp.where(
                lane == tile_lane, pltpu.roll(rows, (tile_lane - (part * pitch + pitch - 1)) % LANES, 1), found
            )
            shifted = pltpu.roll(rows, (offset - part * pitch) % LANES, 1) if offset != part * pitch else rows
            fits = min(window, LANES - offset)
            here = slice(column * LANES, (column + 1) * LANES)
            tags[own, here] = jnp.where((lane >= offset) & (lane < offset + fits), shifted, tags[own, here])
            if fits < window:
                after = slice((column + 1) * LANES, (column + 2) * LANES)
                tags[own, after] = jnp.where(lane < window - fits, shifted, tags[own, after])
    tiles[...] = found.astype(jnp.int32)


def rows_of(window, owner, sorted_ref, tags, tile_at):
    blocks = sorted_ref.shape[0]
    half = tile_at.shape[0]
    part, row = owner // half, owner % half
    row_at = (iota((RQ, blocks * window), 0) + 1).astype(jnp.float32)
    picked = []
    for block in range(blocks):
        tile = tile_at[row, part * blocks + block]
        picked.append(sorted_ref[block, pl.ds(pl.multiple_of(tile * PACK, PACK), window), :])
    matches = one_hot(row_at == tags[pl.ds(owner, 1), : blocks * window])
    return jnp.dot(matches, jnp.concatenate(picked, axis=0), preferred_element_type=jnp.float32)


def tally_kernel(window, samples, data_ref, tail_ref, out_ref, tags, tiles, tile_at, done):
    read_tags(window, data_ref.shape[0], samples, data_ref, tags, tiles)
    copy = pltpu.make_async_copy(tiles, tile_at, done)
    copy.start()
    out_ref[:, RQ:, :] = tail_ref[...]
    copy.wait()

    def per_owner(owner, carry):
        out_ref[owner, :RQ, :] = rows_of(window, owner, data_ref, tags, tile_at).astype(jnp.bfloat16)
        return carry

    lax.fori_loop(0, out_ref.shape[0], per_owner, 0, unroll=4)


def tally_tail_kernel(window, samples, keep, slots, data_ref, out_ref, unfolded, tags, tiles, *rest):
    blocks = data_ref.shape[0]
    half = tiles.shape[1]
    body = samples * keep // PARTS
    tile_at, done = rest[:slots], rest[slots]
    copies = []
    for slot in range(slots):
        read_tags(window, blocks, body + slot * half, data_ref, tags.at[slot], tiles.at[slot])
        copies.append(pltpu.make_async_copy(tiles.at[slot], tile_at[slot], done.at[slot]))
        copies[-1].start()
    for block in range(blocks):
        unfolded[block, :body, :] = data_ref[block, :body, :]
        unfolded[block, body:, :] = unfold(data_ref[block, :body, :].astype(jnp.float32), keep).astype(jnp.bfloat16)
    for copy in copies:
        copy.wait()

    def per_owner(owner, carry):
        rows = rows_of(window, owner, unfolded, tags.at[0], tile_at[0])
        for slot in range(1, slots):
            other = rows_of(window, owner, unfolded, tags.at[slot], tile_at[slot])
            rows = pick(other, PARTS - keep + slot - 1, 1, rows)
        out_ref[owner] = fold(rows, keep).astype(jnp.bfloat16)
        return carry

    lax.fori_loop(0, out_ref.shape[0], per_owner, 0, unroll=2)


def finish_kernel(count, keep, pieces, data_ref, table_ref):
    inner = data_ref.shape[1]
    tails = []
    for at in range(inner):
        total = jnp.sum(data_ref[:, at].astype(jnp.float32), axis=0)
        table_ref[at] = total[:RQ]
        tails.append(jnp.concatenate([total[RQ:], unfold(total[RQ:], keep)], axis=0))
    for at in range(count):
        rows = tails[at]
        for device, _, field, source, target, groups in pieces:
            if field == at:
                rows = pick(shift(tails[count + device], source - target), source, groups, rows)
        table_ref[inner + at] = rows


def local(outer, inner, sample_ids, features, pair_grad):
    samples, vectors, depth = features.shape
    fields = vectors - 1
    owners = outer * inner
    capacity = 2 * samples // owners
    window = min(-(-(PACK - 1 + capacity) // PACK) * PACK, samples)
    extra = owners // HALVES
    tail = fields - inner
    if depth != LANES or not 0 < tail <= inner:
        raise ValueError("unsupported sizes")
    keep, slots, pieces = share_out(tail, inner)
    every = ("tab", "rep")
    groups = [list(range(start, start + inner)) for start in range(0, owners, inner)]
    vmem = pl.BlockSpec(memory_space=pltpu.VMEM)
    params = pltpu.CompilerParams(vmem_limit_bytes=63 * 2**20)
    ids = sample_ids.T
    by_vector = features.transpose(1, 0, 2)
    tail_rows = RQ * keep // PARTS
    tag_shape = (owners, -(-inner * window // LANES) * LANES)

    def send(first, count, is_tail):
        targets = count + 1 - is_tail
        rows = samples * keep // PARTS + slots * extra if is_tail else samples + extra
        shapes = [jax.ShapeDtypeStruct((inner, rows, depth), jnp.bfloat16)]
        specs = [pl.BlockSpec(memory_space=pl.ANY)]
        if not is_tail:
            shapes = [jax.ShapeDtypeStruct((samples, depth), jnp.float32)] + shapes
            specs = [vmem] + specs
        return pl.pallas_call(
            functools.partial(send_kernel, first, count, is_tail, owners, window),
            out_shape=shapes,
            in_specs=[pl.BlockSpec(memory_space=pl.ANY)] * 3,
            out_specs=specs,
            scratch_shapes=[
                pltpu.VMEM(ids.shape, ids.dtype),
                pltpu.VMEM(pair_grad.shape, pair_grad.dtype),
                pltpu.VMEM(by_vector.shape, by_vector.dtype),
                pltpu.VMEM((inner, rows, depth), jnp.bfloat16),
                pltpu.VMEM((count, samples), jnp.float32),
                pltpu.VMEM((count * owners, samples), jnp.bfloat16),
                pltpu.VMEM((samples // SUB, -(-targets // 2), PACK, 2 * LANES), jnp.bfloat16),
                pltpu.VMEM((count, samples, depth), jnp.bfloat16),
                pltpu.SemaphoreType.DMA((3,)),
                pltpu.SemaphoreType.DMA((inner,)),
            ],
            cost_estimate=pl.CostEstimate(
                flops=2 * targets * samples * samples * depth, bytes_accessed=2 * features.size, transcendentals=0
            ),
            compiler_params=params,
            name="send",
        )(ids, pair_grad, by_vector)

    def exchange(blocks, groups):
        return lax.all_to_all(blocks, every, split_axis=0, concat_axis=0, tiled=True, axis_index_groups=groups)

    small = pltpu.CompilerParams(vmem_limit_bytes=28 * 2**20)
    cost = pl.CostEstimate(
        flops=2 * owners * inner * window * RQ * depth, bytes_accessed=4 * inner * samples * depth, transcendentals=0
    )
    arrived_tail = exchange(send(inner, tail, True)[0], groups)
    dense_grad, sent = send(0, inner, False)
    rows_tail = pl.pallas_call(
        functools.partial(tally_tail_kernel, window, samples, keep, slots),
        out_shape=jax.ShapeDtypeStruct((owners, tail_rows, depth), jnp.bfloat16),
        in_specs=[vmem],
        out_specs=vmem,
        scratch_shapes=[
            pltpu.VMEM((inner, samples, depth), jnp.bfloat16),
            pltpu.VMEM((slots,) + tag_shape, jnp.float32),
            pltpu.VMEM((slots, extra, LANES), jnp.int32),
            *[pltpu.SMEM((extra, LANES), jnp.int32)] * slots,
            pltpu.SemaphoreType.DMA((slots,)),
        ],
        cost_estimate=cost,
        compiler_params=small,
        name="tally_tail",
    )(arrived_tail)
    arrived = exchange(sent, groups)
    rows = pl.pallas_call(
        functools.partial(tally_kernel, window, samples),
        out_shape=jax.ShapeDtypeStruct((owners, RQ + tail_rows, depth), jnp.bfloat16),
        in_specs=[vmem] * 2,
        out_specs=vmem,
        scratch_shapes=[
            pltpu.VMEM(tag_shape, jnp.float32),
            pltpu.VMEM((extra, LANES), jnp.int32),
            pltpu.SMEM((extra, LANES), jnp.int32),
            pltpu.SemaphoreType.DMA,
        ],
        cost_estimate=cost,
        compiler_params=small,
        name="tally",
    )(arrived, rows_tail)
    table_grad = pl.pallas_call(
        functools.partial(finish_kernel, tail, keep, pieces),
        out_shape=jax.ShapeDtypeStruct((fields, RQ, depth), jnp.float32),
        in_specs=[vmem],
        out_specs=vmem,
        compiler_params=small,
        name="finish",
    )(exchange(rows, None).reshape(outer, inner, RQ + tail_rows, depth))
    return table_grad, dense_grad


def solution(mesh):
    tab, rep = mesh.shape["tab"], mesh.shape["rep"]
    inner = rep * math.gcd(tab, 4)
    every = ("tab", "rep")
    return jax.shard_map(
        functools.partial(local, tab * rep // inner, inner),
        mesh=mesh,
        in_specs=(P(every, None), P(every, None, None), P(None, every)),
        out_specs=(P(None, every, None), P(every, None)),
        check_vma=False,
    )
```

```python
import functools
import math

import jax
import jax.numpy as jnp
from jax import lax
from jax.experimental import pallas as pl
from jax.experimental.pallas import tpu as pltpu
from jax.sharding import PartitionSpec as P

RQ = 128
LANES = 128
PACK = 16
SUB = 8
HALVES = 2
PARTS = 8
GROUP = LANES // PARTS
GROUP_UNROLL = 16
OWNER_UNROLL = 32
EXACT = 256


def iota(shape, dim):
    return lax.broadcasted_iota(jnp.int32, shape, dim)


def one_hot(hit):
    return jnp.where(hit, 1.0, 0.0).astype(jnp.bfloat16)


def order_fields(first, count, owners, window, ids_ref, store, rank_ref, mine):
    samples = ids_ref.shape[1]
    pitch = LANES // HALVES
    last_tile = (samples - window) // PACK
    for at in range(count):
        own = ids_ref[first + at : first + at + 1, :] // RQ
        mine[at * owners : (at + 1) * owners, :] = one_hot(iota((owners, samples), 0) == own)
    earlier = one_hot(iota((samples, samples), 0) < iota((samples, samples), 1))
    before = jnp.dot(mine[...], earlier, preferred_element_type=jnp.float32)
    held = jnp.dot(mine[...], jnp.ones((samples, LANES), jnp.bfloat16), preferred_element_type=jnp.float32)
    below = one_hot(iota((owners, owners), 0) > iota((owners, owners), 1))
    slot_at = iota((LANES, samples), 0).astype(jnp.float32)
    lane = iota((owners // HALVES, LANES), 1)
    starts = [
        jnp.dot(below, held[at * owners : (at + 1) * owners].astype(jnp.bfloat16), preferred_element_type=jnp.float32)
        for at in range(count)
    ]
    placed = []
    for at, start in enumerate(starts):
        rows = slice(at * owners, (at + 1) * owners)
        tile = jnp.minimum(jnp.floor(start * (1.0 / PACK)), float(last_tile))
        hit = mine[rows, :].astype(jnp.float32)
        place = hit * (before[rows] + jnp.concatenate([start] * (samples // LANES), axis=1))
        base = hit * jnp.concatenate([tile * PACK] * (samples // LANES), axis=1)
        rank = jnp.sum(place, axis=0, keepdims=True)
        slot = rank - jnp.sum(base, axis=0, keepdims=True)
        rank_ref[at : at + 1, :] = rank
        placed.append((tile, slot))
    for at, (tile, slot) in enumerate(placed):
        hit = mine[at * owners : (at + 1) * owners, :].astype(jnp.float32)
        tag = (ids_ref[first + at : first + at + 1, :] % RQ + 1).astype(jnp.float32)
        tags = lax.dot_general(
            (hit * tag).astype(jnp.bfloat16),
            one_hot(slot_at == slot),
            (((1,), (1,)), ((), ())),
            preferred_element_type=jnp.float32,
        )
        half = owners // HALVES
        row = tags[:half] + pltpu.roll(tags[half:], pitch, 1)
        row = jnp.where(lane == pitch - 1, tile[:half], jnp.where(lane == LANES - 1, tile[half:], row))
        store(at, row.astype(jnp.bfloat16))


def lane_group(rows):
    return iota((rows, LANES), 1) // GROUP


def shift(block, groups):
    return pltpu.roll(block, groups * GROUP % LANES, 1) if groups % PARTS else block


def pick(block, first, count, other):
    group = lane_group(block.shape[0])
    return jnp.where((group >= first) & (group < first + count), block, other)


def fold(block, keep):
    rows = block.shape[0] // PARTS
    out = []
    for part in range(keep):
        kept = block[part * rows : (part + 1) * rows]
        for at in range(keep, PARTS):
            kept = pick(shift(block[at * rows : (at + 1) * rows], at - part), at, 1, kept)
        out.append(kept)
    return jnp.concatenate(out, axis=0)


def unfold(block, keep):
    rows = block.shape[0] // keep
    out = []
    for at in range(keep, PARTS):
        moved = jnp.zeros((rows, LANES), block.dtype)
        for part in range(keep):
            moved = pick(shift(block[part * rows : (part + 1) * rows], part - at), part, 1, moved)
        out.append(moved)
    return jnp.concatenate(out, axis=0)


def share_out(count, devices):
    keep = -(-count * PARTS // devices)
    rest, others = PARTS - keep, devices - count
    singles = keep - rest
    if singles < 0 or (count - others) * rest > others * singles:
        raise ValueError("unsupported sizes")
    pieces = [(at, 0, at, keep, 0, rest) for at in range(min(others, count))]
    for at in range(max(count - others, 0) * rest):
        slot = at % singles
        pieces.append((at // singles, 1 + slot, others + at // rest, keep + at % rest, rest + slot, 1))
    return keep, 1 + singles, pieces


def send_kernel(first, count, tail, owners, window, ids_hbm, pairs_hbm, feat_hbm, *rest):
    if tail:
        payload_hbm, *rest = rest
    else:
        dense_ref, payload_hbm, *rest = rest
    ids_ref, pairs_ref, feat_ref, payload_ref, rank_ref, mine, weights, grads, in_done, out_done = rest
    inputs = [
        pltpu.make_async_copy(source, target, in_done.at[at])
        for at, (source, target) in enumerate([(ids_hbm, ids_ref), (pairs_hbm, pairs_ref), (feat_hbm, feat_ref)])
    ]
    for copy in inputs:
        copy.start()

    def leave(at):
        return pltpu.make_async_copy(payload_ref.at[at], payload_hbm.at[at], out_done.at[at])

    vectors, samples, depth = feat_ref.shape
    span = 2 * LANES
    keep, slots, pieces = share_out(count, payload_ref.shape[0]) if tail else (PARTS, 1, [])
    body = samples * keep // PARTS
    extra = owners // HALVES
    for at in range(count, payload_ref.shape[0]):
        payload_ref[at, body:] = jnp.zeros((payload_ref.shape[1] - body, LANES), jnp.bfloat16)

    def store(at, row):
        homes = [(at, slot) for slot in range(slots)]
        homes += [(count + device, slot) for device, slot, field, *_ in pieces if field == at]
        for device, slot in homes:
            payload_ref[device, body + slot * extra : body + (slot + 1) * extra, :] = row

    inputs[0].wait()
    inputs[1].wait()
    order_fields(first, count, owners, window, ids_ref, store, rank_ref, mine)
    targets = ([] if tail else [0]) + list(range(first + 1, first + 1 + count))
    pairs = pairs_ref[...].astype(jnp.float32).T.astype(jnp.bfloat16)
    pair_at = iota((pairs.shape[1], span), 0)
    source = iota((1, span), 1) // SUB
    own_lane = one_hot(iota((PACK, span), 1) % SUB == iota((PACK, span), 0) % SUB)

    def spread_of(target):
        pair = jnp.where(source < target, target * (target - 1) // 2 + source, source * (source - 1) // 2 + target)
        pair = jnp.where((source == target) | (source >= vectors), -1, pair)
        found = jnp.dot(pairs, one_hot(pair_at == pair), preferred_element_type=jnp.float32)
        return found.reshape(samples // SUB, SUB, span)

    for at in range(0, len(targets), 2):
        low = spread_of(targets[at])
        high = spread_of(targets[at + 1]) if at + 1 < len(targets) else jnp.zeros_like(low)
        weights[:, at // 2] = jnp.concatenate([low, high], axis=1).astype(jnp.bfloat16) * own_lane
    inputs[2].wait()

    def per_group(group, carry):
        begin = pl.multiple_of(group * PACK, PACK)
        block = feat_ref[:, pl.ds(begin, PACK), :].astype(jnp.float32)
        outs = []
        for part in range(PACK // SUB):
            right = block[:, part * SUB : (part + 1) * SUB, :].reshape(vectors * SUB, depth)
            right = jnp.concatenate([right, jnp.zeros((span - vectors * SUB, depth), jnp.float32)], axis=0)
            left = weights[group * (PACK // SUB) + part].reshape(-1, span)
            out = jnp.dot(left, right.astype(jnp.bfloat16), preferred_element_type=jnp.float32)
            outs.append(out.reshape(-1, SUB, depth))
        out = jnp.concatenate(outs, axis=1)
        if not tail:
            dense_ref[pl.ds(begin, PACK), :] = out[0]
            out = out[1:]
        grads[:, pl.ds(begin, PACK), :] = out[:count].astype(jnp.bfloat16)
        return carry

    lax.fori_loop(0, samples // PACK, per_group, 0, unroll=GROUP_UNROLL)
    near = math.gcd(samples, EXACT)
    slot_at = iota((near, samples), 0).astype(jnp.float32).astype(jnp.bfloat16)

    def placed(at):
        rank = rank_ref[pl.ds(at, 1), :]
        tiles = []
        for top in range(0, samples, near):
            here = jnp.broadcast_to((rank - top).astype(jnp.bfloat16), (near, samples))
            tiles.append(jnp.where(slot_at == here, jnp.bfloat16(1), jnp.bfloat16(0)))
        placing = jnp.concatenate(tiles, axis=0)
        return jnp.dot(placing, grads[at], preferred_element_type=jnp.float32)

    if tail:
        for at in range(count):
            block = placed(at)
            grads[at] = block.astype(jnp.bfloat16)
            payload_ref[at, :body, :] = fold(block, keep).astype(jnp.bfloat16)
            leave(at).start()
        for at in range(payload_ref.shape[0] - count):
            block = jnp.zeros((samples, LANES), jnp.float32)
            for device, _, field, source, target, groups in pieces:
                if device == at:
                    block = pick(shift(grads[field].astype(jnp.float32), target - source), target, groups, block)
            payload_ref[count + at, :body, :] = fold(block, keep).astype(jnp.bfloat16)
            leave(count + at).start()
    else:

        def per_field(at, carry):
            payload_ref[at, :body, :] = placed(at).astype(jnp.bfloat16)
            leave(at).start()
            return carry

        lax.fori_loop(0, count, per_field, 0, unroll=2)
    for at in range(payload_ref.shape[0]):
        leave(at).wait()


def read_tags(window, blocks, first_row, data_ref, tags, tiles):
    half, pitch = tiles.shape[0], LANES // HALVES
    lane = iota((half, LANES), 1)
    tags[...] = jnp.zeros_like(tags)
    found = jnp.zeros((half, LANES), jnp.float32)
    for block in range(blocks):
        rows = data_ref[block, first_row : first_row + half, :].astype(jnp.float32)
        column, offset = divmod(block * window, LANES)
        for part in range(HALVES):
            own = slice(part * half, (part + 1) * half)
            tile_lane = part * blocks + block
            found = jnp.where(
                lane == tile_lane, pltpu.roll(rows, (tile_lane - (part * pitch + pitch - 1)) % LANES, 1), found
            )
            shifted = pltpu.roll(rows, (offset - part * pitch) % LANES, 1) if offset != part * pitch else rows
            fits = min(window, LANES - offset)
            here = slice(column * LANES, (column + 1) * LANES)
            tags[own, here] = jnp.where((lane >= offset) & (lane < offset + fits), shifted, tags[own, here])
            if fits < window:
                after = slice((column + 1) * LANES, (column + 2) * LANES)
                tags[own, after] = jnp.where(lane < window - fits, shifted, tags[own, after])
    tiles[...] = found.astype(jnp.int32)


def rows_of(window, owner, sorted_ref, tags, tile_at):
    blocks = sorted_ref.shape[0]
    half = tile_at.shape[0]
    part, row = owner // half, owner % half
    row_at = (iota((RQ, blocks * window), 0) + 1).astype(jnp.float32)
    picked = []
    for block in range(blocks):
        tile = tile_at[row, part * blocks + block]
        picked.append(sorted_ref[block, pl.ds(pl.multiple_of(tile * PACK, PACK), window), :])
    matches = one_hot(row_at == tags[pl.ds(owner, 1), : blocks * window])
    return jnp.dot(matches, jnp.concatenate(picked, axis=0), preferred_element_type=jnp.float32)


def tally_kernel(window, samples, data_ref, tail_ref, out_ref, tags, tiles, tile_at, done):
    read_tags(window, data_ref.shape[0], samples, data_ref, tags, tiles)
    copy = pltpu.make_async_copy(tiles, tile_at, done)
    copy.start()
    out_ref[:, RQ:, :] = tail_ref[...]
    copy.wait()

    def per_owner(owner, carry):
        out_ref[owner, :RQ, :] = rows_of(window, owner, data_ref, tags, tile_at).astype(jnp.bfloat16)
        return carry

    lax.fori_loop(0, out_ref.shape[0], per_owner, 0, unroll=OWNER_UNROLL)


def tally_tail_kernel(window, samples, keep, slots, data_ref, out_ref, unfolded, tags, tiles, *rest):
    blocks = data_ref.shape[0]
    half = tiles.shape[1]
    body = samples * keep // PARTS
    tile_at, done = rest[:slots], rest[slots]
    copies = []
    for slot in range(slots):
        read_tags(window, blocks, body + slot * half, data_ref, tags.at[slot], tiles.at[slot])
        copies.append(pltpu.make_async_copy(tiles.at[slot], tile_at[slot], done.at[slot]))
        copies[-1].start()
    for block in range(blocks):
        unfolded[block, :body, :] = data_ref[block, :body, :]
        unfolded[block, body:, :] = unfold(data_ref[block, :body, :].astype(jnp.float32), keep).astype(jnp.bfloat16)
    for copy in copies:
        copy.wait()

    def per_owner(owner, carry):
        rows = rows_of(window, owner, unfolded, tags.at[0], tile_at[0])
        for slot in range(1, slots):
            other = rows_of(window, owner, unfolded, tags.at[slot], tile_at[slot])
            rows = pick(other, PARTS - keep + slot - 1, 1, rows)
        out_ref[owner] = fold(rows, keep).astype(jnp.bfloat16)
        return carry

    lax.fori_loop(0, out_ref.shape[0], per_owner, 0, unroll=2)


def finish_kernel(count, keep, pieces, data_ref, table_hbm, table_ref, done):
    inner = data_ref.shape[1]
    tails = []

    def leave(at):
        return pltpu.make_async_copy(table_ref.at[at], table_hbm.at[at], done.at[at])

    for at in range(inner):
        total = jnp.sum(data_ref[:, at].astype(jnp.float32), axis=0)
        table_ref[at] = total[:RQ]
        leave(at).start()
        tails.append(jnp.concatenate([total[RQ:], unfold(total[RQ:], keep)], axis=0))
    for at in range(count):
        rows = tails[at]
        for device, _, field, source, target, groups in pieces:
            if field == at:
                rows = pick(shift(tails[count + device], source - target), source, groups, rows)
        table_ref[inner + at] = rows
        leave(inner + at).start()
    for at in range(table_ref.shape[0]):
        leave(at).wait()


def local(outer, inner, sample_ids, features, pair_grad):
    samples, vectors, depth = features.shape
    fields = vectors - 1
    owners = outer * inner
    capacity = 2 * samples // owners
    window = min(-(-(PACK - 1 + capacity) // PACK) * PACK, samples)
    extra = owners // HALVES
    tail = fields - inner
    if depth != LANES or not 0 < tail <= inner:
        raise ValueError("unsupported sizes")
    keep, slots, pieces = share_out(tail, inner)
    every = ("tab", "rep")
    groups = [list(range(start, start + inner)) for start in range(0, owners, inner)]
    vmem = pl.BlockSpec(memory_space=pltpu.VMEM)
    params = pltpu.CompilerParams(vmem_limit_bytes=63 * 2**20)
    ids = sample_ids.T
    by_vector = features.transpose(1, 0, 2)
    tail_rows = RQ * keep // PARTS
    tag_shape = (owners, -(-inner * window // LANES) * LANES)

    def send(first, count, is_tail):
        targets = count + 1 - is_tail
        rows = samples * keep // PARTS + slots * extra if is_tail else samples + extra
        shapes = [jax.ShapeDtypeStruct((inner, rows, depth), jnp.bfloat16)]
        specs = [pl.BlockSpec(memory_space=pl.ANY)]
        if not is_tail:
            shapes = [jax.ShapeDtypeStruct((samples, depth), jnp.float32)] + shapes
            specs = [vmem] + specs
        return pl.pallas_call(
            functools.partial(send_kernel, first, count, is_tail, owners, window),
            out_shape=shapes,
            in_specs=[pl.BlockSpec(memory_space=pl.ANY)] * 3,
            out_specs=specs,
            scratch_shapes=[
                pltpu.VMEM(ids.shape, ids.dtype),
                pltpu.VMEM(pair_grad.shape, pair_grad.dtype),
                pltpu.VMEM(by_vector.shape, by_vector.dtype),
                pltpu.VMEM((inner, rows, depth), jnp.bfloat16),
                pltpu.VMEM((count, samples), jnp.float32),
                pltpu.VMEM((count * owners, samples), jnp.bfloat16),
                pltpu.VMEM((samples // SUB, -(-targets // 2), PACK, 2 * LANES), jnp.bfloat16),
                pltpu.VMEM((count, samples, depth), jnp.bfloat16),
                pltpu.SemaphoreType.DMA((3,)),
                pltpu.SemaphoreType.DMA((inner,)),
            ],
            cost_estimate=pl.CostEstimate(
                flops=2 * targets * samples * samples * depth, bytes_accessed=2 * features.size, transcendentals=0
            ),
            compiler_params=params,
            name="send",
        )(ids, pair_grad, by_vector)

    def exchange(blocks, groups):
        return lax.all_to_all(blocks, every, split_axis=0, concat_axis=0, tiled=True, axis_index_groups=groups)

    small = pltpu.CompilerParams(vmem_limit_bytes=28 * 2**20)
    cost = pl.CostEstimate(
        flops=2 * owners * inner * window * RQ * depth, bytes_accessed=4 * inner * samples * depth, transcendentals=0
    )
    arrived_tail = exchange(send(inner, tail, True)[0], groups)
    dense_grad, sent = send(0, inner, False)
    rows_tail = pl.pallas_call(
        functools.partial(tally_tail_kernel, window, samples, keep, slots),
        out_shape=jax.ShapeDtypeStruct((owners, tail_rows, depth), jnp.bfloat16),
        in_specs=[vmem],
        out_specs=vmem,
        scratch_shapes=[
            pltpu.VMEM((inner, samples, depth), jnp.bfloat16),
            pltpu.VMEM((slots,) + tag_shape, jnp.float32),
            pltpu.VMEM((slots, extra, LANES), jnp.int32),
            *[pltpu.SMEM((extra, LANES), jnp.int32)] * slots,
            pltpu.SemaphoreType.DMA((slots,)),
        ],
        cost_estimate=cost,
        compiler_params=small,
        name="tally_tail",
    )(arrived_tail)
    arrived = exchange(sent, groups)
    rows = pl.pallas_call(
        functools.partial(tally_kernel, window, samples),
        out_shape=jax.ShapeDtypeStruct((owners, RQ + tail_rows, depth), jnp.bfloat16),
        in_specs=[vmem] * 2,
        out_specs=vmem,
        scratch_shapes=[
            pltpu.VMEM(tag_shape, jnp.float32),
            pltpu.VMEM((extra, LANES), jnp.int32),
            pltpu.SMEM((extra, LANES), jnp.int32),
            pltpu.SemaphoreType.DMA,
        ],
        cost_estimate=cost,
        compiler_params=small,
        name="tally",
    )(arrived, rows_tail)
    table_grad = pl.pallas_call(
        functools.partial(finish_kernel, tail, keep, pieces),
        out_shape=jax.ShapeDtypeStruct((fields, RQ, depth), jnp.float32),
        in_specs=[vmem],
        out_specs=pl.BlockSpec(memory_space=pl.ANY),
        scratch_shapes=[pltpu.VMEM((fields, RQ, depth), jnp.float32), pltpu.SemaphoreType.DMA((fields,))],
        compiler_params=small,
        name="finish",
    )(exchange(rows, None).reshape(outer, inner, RQ + tail_rows, depth))
    return table_grad, dense_grad


def solution(mesh):
    tab, rep = mesh.shape["tab"], mesh.shape["rep"]
    inner = rep * math.gcd(tab, 4)
    every = ("tab", "rep")
    return jax.shard_map(
        functools.partial(local, tab * rep // inner, inner),
        mesh=mesh,
        in_specs=(P(every, None), P(every, None, None), P(None, every)),
        out_specs=(P(None, every, None), P(every, None)),
        check_vma=False,
    )
```

```python
import functools
import math

import jax
import jax.numpy as jnp
from jax import lax
from jax.experimental import pallas as pl
from jax.experimental.pallas import tpu as pltpu
from jax.sharding import PartitionSpec as P

RQ = 128
LANES = 128
PACK = 16
SUB = 8
HALVES = 2
PARTS = 8
GROUP = LANES // PARTS
GROUP_UNROLL = 32
OWNER_UNROLL = 32
EXACT = 256


def iota(shape, dim):
    return lax.broadcasted_iota(jnp.int32, shape, dim)


def one_hot(hit):
    return jnp.where(hit, 1.0, 0.0).astype(jnp.bfloat16)


def order_fields(first, count, owners, window, ids_ref, store, rank_ref, mine):
    samples = ids_ref.shape[1]
    pitch = LANES // HALVES
    last_tile = (samples - window) // PACK
    for at in range(count):
        own = ids_ref[first + at : first + at + 1, :] // RQ
        mine[at * owners : (at + 1) * owners, :] = one_hot(iota((owners, samples), 0) == own)
    earlier = one_hot(iota((samples, samples), 0) < iota((samples, samples), 1))
    before = jnp.dot(mine[...], earlier, preferred_element_type=jnp.float32)
    held = jnp.dot(mine[...], jnp.ones((samples, LANES), jnp.bfloat16), preferred_element_type=jnp.float32)
    below = one_hot(iota((owners, owners), 0) > iota((owners, owners), 1))
    slot_at = iota((LANES, samples), 0).astype(jnp.float32)
    lane = iota((owners // HALVES, LANES), 1)
    starts = [
        jnp.dot(below, held[at * owners : (at + 1) * owners].astype(jnp.bfloat16), preferred_element_type=jnp.float32)
        for at in range(count)
    ]
    placed = []
    for at, start in enumerate(starts):
        rows = slice(at * owners, (at + 1) * owners)
        tile = jnp.minimum(jnp.floor(start * (1.0 / PACK)), float(last_tile))
        hit = mine[rows, :].astype(jnp.float32)
        place = hit * (before[rows] + jnp.concatenate([start] * (samples // LANES), axis=1))
        base = hit * jnp.concatenate([tile * PACK] * (samples // LANES), axis=1)
        rank = jnp.sum(place, axis=0, keepdims=True)
        slot = rank - jnp.sum(base, axis=0, keepdims=True)
        rank_ref[at : at + 1, :] = rank
        placed.append((tile, slot))
    for at, (tile, slot) in enumerate(placed):
        hit = mine[at * owners : (at + 1) * owners, :].astype(jnp.float32)
        tag = (ids_ref[first + at : first + at + 1, :] % RQ + 1).astype(jnp.float32)
        tags = lax.dot_general(
            (hit * tag).astype(jnp.bfloat16),
            one_hot(slot_at == slot),
            (((1,), (1,)), ((), ())),
            preferred_element_type=jnp.float32,
        )
        half = owners // HALVES
        row = tags[:half] + pltpu.roll(tags[half:], pitch, 1)
        row = jnp.where(lane == pitch - 1, tile[:half], jnp.where(lane == LANES - 1, tile[half:], row))
        store(at, row.astype(jnp.bfloat16))


def lane_group(rows):
    return iota((rows, LANES), 1) // GROUP


def shift(block, groups):
    return pltpu.roll(block, groups * GROUP % LANES, 1) if groups % PARTS else block


def pick(block, first, count, other):
    group = lane_group(block.shape[0])
    return jnp.where((group >= first) & (group < first + count), block, other)


def fold(block, keep):
    rows = block.shape[0] // PARTS
    out = []
    for part in range(keep):
        kept = block[part * rows : (part + 1) * rows]
        for at in range(keep, PARTS):
            kept = pick(shift(block[at * rows : (at + 1) * rows], at - part), at, 1, kept)
        out.append(kept)
    return jnp.concatenate(out, axis=0)


def unfold(block, keep):
    rows = block.shape[0] // keep
    out = []
    for at in range(keep, PARTS):
        moved = jnp.zeros((rows, LANES), block.dtype)
        for part in range(keep):
            moved = pick(shift(block[part * rows : (part + 1) * rows], part - at), part, 1, moved)
        out.append(moved)
    return jnp.concatenate(out, axis=0)


def share_out(count, devices):
    keep = -(-count * PARTS // devices)
    rest, others = PARTS - keep, devices - count
    singles = keep - rest
    if singles < 0 or (count - others) * rest > others * singles:
        raise ValueError("unsupported sizes")
    pieces = [(at, 0, at, keep, 0, rest) for at in range(min(others, count))]
    for at in range(max(count - others, 0) * rest):
        slot = at % singles
        pieces.append((at // singles, 1 + slot, others + at // rest, keep + at % rest, rest + slot, 1))
    return keep, 1 + singles, pieces


def send_kernel(first, count, tail, owners, window, me_ref, ids_hbm, pairs_hbm, feat_hbm, *rest):
    if tail:
        payload_hbm, *rest = rest
    else:
        dense_ref, *rest = rest
        payload_hbm, rest = rest[:count], rest[count:]
    ids_ref, pairs_ref, feat_ref, payload_ref, rank_ref, mine, weights, grads, in_done, out_done = rest
    inputs = [
        pltpu.make_async_copy(source, target, in_done.at[at])
        for at, (source, target) in enumerate([(ids_hbm, ids_ref), (pairs_hbm, pairs_ref), (feat_hbm, feat_ref)])
    ]
    for copy in inputs:
        copy.start()

    def leave(at, hop=0):
        target = payload_hbm.at[at] if tail else payload_hbm[hop]
        return pltpu.make_async_copy(payload_ref.at[at], target, out_done.at[at])

    vectors, samples, depth = feat_ref.shape
    span = 2 * LANES
    keep, slots, pieces = share_out(count, payload_ref.shape[0]) if tail else (PARTS, 1, [])
    body = samples * keep // PARTS
    extra = owners // HALVES
    for at in range(count, payload_ref.shape[0]):
        payload_ref[at, body:] = jnp.zeros((payload_ref.shape[1] - body, LANES), jnp.bfloat16)

    def store(at, row):
        homes = [(at, slot) for slot in range(slots)]
        homes += [(count + device, slot) for device, slot, field, *_ in pieces if field == at]
        for device, slot in homes:
            payload_ref[device, body + slot * extra : body + (slot + 1) * extra, :] = row

    inputs[0].wait()
    inputs[1].wait()
    order_fields(first, count, owners, window, ids_ref, store, rank_ref, mine)
    targets = ([] if tail else [0]) + list(range(first + 1, first + 1 + count))
    pairs = pairs_ref[...].astype(jnp.float32).T.astype(jnp.bfloat16)
    pair_at = iota((pairs.shape[1], span), 0)
    source = iota((1, span), 1) // SUB
    own_lane = one_hot(iota((PACK, span), 1) % SUB == iota((PACK, span), 0) % SUB)

    def spread_of(target):
        pair = jnp.where(source < target, target * (target - 1) // 2 + source, source * (source - 1) // 2 + target)
        pair = jnp.where((source == target) | (source >= vectors), -1, pair)
        found = jnp.dot(pairs, one_hot(pair_at == pair), preferred_element_type=jnp.float32)
        return found.reshape(samples // SUB, SUB, span)

    for at in range(0, len(targets), 2):
        low = spread_of(targets[at])
        high = spread_of(targets[at + 1]) if at + 1 < len(targets) else jnp.zeros_like(low)
        weights[:, at // 2] = jnp.concatenate([low, high], axis=1).astype(jnp.bfloat16) * own_lane
    inputs[2].wait()

    def per_group(group, carry):
        begin = pl.multiple_of(group * PACK, PACK)
        block = feat_ref[:, pl.ds(begin, PACK), :].astype(jnp.float32)
        outs = []
        for part in range(PACK // SUB):
            right = block[:, part * SUB : (part + 1) * SUB, :].reshape(vectors * SUB, depth)
            right = jnp.concatenate([right, jnp.zeros((span - vectors * SUB, depth), jnp.float32)], axis=0)
            left = weights[group * (PACK // SUB) + part].reshape(-1, span)
            out = jnp.dot(left, right.astype(jnp.bfloat16), preferred_element_type=jnp.float32)
            outs.append(out.reshape(-1, SUB, depth))
        out = jnp.concatenate(outs, axis=1)
        if not tail:
            dense_ref[pl.ds(begin, PACK), :] = out[0]
            out = out[1:]
        grads[:, pl.ds(begin, PACK), :] = out[:count].astype(jnp.bfloat16)
        return carry

    lax.fori_loop(0, samples // PACK, per_group, 0, unroll=GROUP_UNROLL)
    near = math.gcd(samples, EXACT)
    slot_at = iota((near, samples), 0).astype(jnp.float32).astype(jnp.bfloat16)

    def placed(at):
        rank = rank_ref[pl.ds(at, 1), :]
        tiles = []
        for top in range(0, samples, near):
            here = jnp.broadcast_to((rank - top).astype(jnp.bfloat16), (near, samples))
            tiles.append(jnp.where(slot_at == here, jnp.bfloat16(1), jnp.bfloat16(0)))
        placing = jnp.concatenate(tiles, axis=0)
        return jnp.dot(placing, grads[at], preferred_element_type=jnp.float32)

    if tail:
        for at in range(count):
            block = placed(at)
            grads[at] = block.astype(jnp.bfloat16)
            payload_ref[at, :body, :] = fold(block, keep).astype(jnp.bfloat16)
            leave(at).start()
        for at in range(payload_ref.shape[0] - count):
            block = jnp.zeros((samples, LANES), jnp.float32)
            for device, _, field, source, target, groups in pieces:
                if device == at:
                    block = pick(shift(grads[field].astype(jnp.float32), target - source), target, groups, block)
            payload_ref[count + at, :body, :] = fold(block, keep).astype(jnp.bfloat16)
            leave(count + at).start()
    else:

        def per_field(at, carry):
            payload_ref[at, :body, :] = placed(at).astype(jnp.bfloat16)
            for hop in range(count):
                pl.when(lax.bitwise_xor(me_ref[0], at) == hop)(leave(at, hop).start)
            return carry

        lax.fori_loop(0, count, per_field, 0, unroll=2)
    for at in range(payload_ref.shape[0]):
        leave(at).wait()


def read_tags(window, blocks, first_row, data_ref, tags, tiles):
    half, pitch = tiles.shape[0], LANES // HALVES
    lane = iota((half, LANES), 1)
    tags[...] = jnp.zeros_like(tags)
    found = jnp.zeros((half, LANES), jnp.float32)
    for block in range(blocks):
        rows = data_ref[block][first_row : first_row + half, :].astype(jnp.float32)
        column, offset = divmod(block * window, LANES)
        for part in range(HALVES):
            own = slice(part * half, (part + 1) * half)
            tile_lane = part * blocks + block
            found = jnp.where(
                lane == tile_lane, pltpu.roll(rows, (tile_lane - (part * pitch + pitch - 1)) % LANES, 1), found
            )
            shifted = pltpu.roll(rows, (offset - part * pitch) % LANES, 1) if offset != part * pitch else rows
            fits = min(window, LANES - offset)
            here = slice(column * LANES, (column + 1) * LANES)
            tags[own, here] = jnp.where((lane >= offset) & (lane < offset + fits), shifted, tags[own, here])
            if fits < window:
                after = slice((column + 1) * LANES, (column + 2) * LANES)
                tags[own, after] = jnp.where(lane < window - fits, shifted, tags[own, after])
    tiles[...] = found.astype(jnp.int32)


def rows_of(window, owner, sorted_ref, tags, tile_at):
    blocks = len(sorted_ref)
    half = tile_at.shape[0]
    part, row = owner // half, owner % half
    row_at = (iota((RQ, blocks * window), 0) + 1).astype(jnp.float32)
    picked = []
    for block in range(blocks):
        tile = tile_at[row, part * blocks + block]
        picked.append(sorted_ref[block][pl.ds(pl.multiple_of(tile * PACK, PACK), window), :])
    matches = one_hot(row_at == tags[pl.ds(owner, 1), : blocks * window])
    return jnp.dot(matches, jnp.concatenate(picked, axis=0), preferred_element_type=jnp.float32)


def tally_kernel(window, samples, tail_ref, *rest):
    *data_ref, out_ref, tags, tiles, tile_at, done = rest
    read_tags(window, len(data_ref), samples, data_ref, tags, tiles)
    copy = pltpu.make_async_copy(tiles, tile_at, done)
    copy.start()
    out_ref[:, RQ:, :] = tail_ref[...]
    copy.wait()

    def per_owner(owner, carry):
        out_ref[owner, :RQ, :] = rows_of(window, owner, data_ref, tags, tile_at).astype(jnp.bfloat16)
        return carry

    lax.fori_loop(0, out_ref.shape[0], per_owner, 0, unroll=OWNER_UNROLL)


def tally_tail_kernel(window, samples, keep, slots, data_ref, out_ref, unfolded, tags, tiles, *rest):
    blocks = data_ref.shape[0]
    half = tiles.shape[1]
    body = samples * keep // PARTS
    tile_at, done = rest[:slots], rest[slots]
    copies = []
    for slot in range(slots):
        read_tags(window, blocks, body + slot * half, [data_ref.at[at] for at in range(blocks)], tags.at[slot], tiles.at[slot])
        copies.append(pltpu.make_async_copy(tiles.at[slot], tile_at[slot], done.at[slot]))
        copies[-1].start()
    for block in range(blocks):
        unfolded[block, :body, :] = data_ref[block, :body, :]
        unfolded[block, body:, :] = unfold(data_ref[block, :body, :].astype(jnp.float32), keep).astype(jnp.bfloat16)
    for copy in copies:
        copy.wait()

    ordered = [unfolded.at[at] for at in range(blocks)]

    def per_owner(owner, carry):
        rows = rows_of(window, owner, ordered, tags.at[0], tile_at[0])
        for slot in range(1, slots):
            other = rows_of(window, owner, ordered, tags.at[slot], tile_at[slot])
            rows = pick(other, PARTS - keep + slot - 1, 1, rows)
        out_ref[owner] = fold(rows, keep).astype(jnp.bfloat16)
        return carry

    lax.fori_loop(0, out_ref.shape[0], per_owner, 0, unroll=2)


def finish_kernel(count, keep, pieces, data_ref, table_hbm, table_ref, done):
    inner = data_ref.shape[1]
    tails = []

    def leave(at):
        return pltpu.make_async_copy(table_ref.at[at], table_hbm.at[at], done.at[at])

    for at in range(inner):
        total = jnp.sum(data_ref[:, at].astype(jnp.float32), axis=0)
        table_ref[at] = total[:RQ]
        leave(at).start()
        tails.append(jnp.concatenate([total[RQ:], unfold(total[RQ:], keep)], axis=0))
    for at in range(count):
        rows = tails[at]
        for device, _, field, source, target, groups in pieces:
            if field == at:
                rows = pick(shift(tails[count + device], source - target), source, groups, rows)
        table_ref[inner + at] = rows
        leave(inner + at).start()
    for at in range(table_ref.shape[0]):
        leave(at).wait()


def local(outer, inner, sample_ids, features, pair_grad):
    samples, vectors, depth = features.shape
    fields = vectors - 1
    owners = outer * inner
    capacity = 2 * samples // owners
    window = min(-(-(PACK - 1 + capacity) // PACK) * PACK, samples)
    extra = owners // HALVES
    tail = fields - inner
    if depth != LANES or not 0 < tail <= inner:
        raise ValueError("unsupported sizes")
    keep, slots, pieces = share_out(tail, inner)
    every = ("tab", "rep")
    groups = [list(range(start, start + inner)) for start in range(0, owners, inner)]
    vmem = pl.BlockSpec(memory_space=pltpu.VMEM)
    params = pltpu.CompilerParams(vmem_limit_bytes=63 * 2**20)
    ids = sample_ids.T
    by_vector = features.transpose(1, 0, 2)
    me = jnp.reshape(lax.axis_index(every) % inner, (1,))
    tail_rows = RQ * keep // PARTS
    tag_shape = (owners, -(-inner * window // LANES) * LANES)

    def send(first, count, is_tail):
        targets = count + 1 - is_tail
        rows = samples * keep // PARTS + slots * extra if is_tail else samples + extra
        shapes = [jax.ShapeDtypeStruct((inner, rows, depth), jnp.bfloat16)]
        specs = [pl.BlockSpec(memory_space=pl.ANY)]
        if not is_tail:
            shapes = [jax.ShapeDtypeStruct((samples, depth), jnp.float32)]
            shapes += [jax.ShapeDtypeStruct((rows, depth), jnp.bfloat16)] * inner
            specs = [vmem] + specs * inner
        return pl.pallas_call(
            functools.partial(send_kernel, first, count, is_tail, owners, window),
            out_shape=shapes,
            in_specs=[pl.BlockSpec(memory_space=pltpu.SMEM)] + [pl.BlockSpec(memory_space=pl.ANY)] * 3,
            out_specs=specs,
            scratch_shapes=[
                pltpu.VMEM(ids.shape, ids.dtype),
                pltpu.VMEM(pair_grad.shape, pair_grad.dtype),
                pltpu.VMEM(by_vector.shape, by_vector.dtype),
                pltpu.VMEM((inner, rows, depth), jnp.bfloat16),
                pltpu.VMEM((count, samples), jnp.float32),
                pltpu.VMEM((count * owners, samples), jnp.bfloat16),
                pltpu.VMEM((samples // SUB, -(-targets // 2), PACK, 2 * LANES), jnp.bfloat16),
                pltpu.VMEM((count, samples, depth), jnp.bfloat16),
                pltpu.SemaphoreType.DMA((3,)),
                pltpu.SemaphoreType.DMA((inner,)),
            ],
            cost_estimate=pl.CostEstimate(
                flops=2 * targets * samples * samples * depth, bytes_accessed=2 * features.size, transcendentals=0
            ),
            compiler_params=params,
            name="send",
        )(me, ids, pair_grad, by_vector)

    def exchange(blocks, groups):
        return lax.all_to_all(blocks, every, split_axis=0, concat_axis=0, tiled=True, axis_index_groups=groups)

    small = pltpu.CompilerParams(vmem_limit_bytes=28 * 2**20)
    cost = pl.CostEstimate(
        flops=2 * owners * inner * window * RQ * depth, bytes_accessed=4 * inner * samples * depth, transcendentals=0
    )
    arrived_tail = exchange(send(inner, tail, True)[0], groups)
    dense_grad, *sent = send(0, inner, False)
    rows_tail = pl.pallas_call(
        functools.partial(tally_tail_kernel, window, samples, keep, slots),
        out_shape=jax.ShapeDtypeStruct((owners, tail_rows, depth), jnp.bfloat16),
        in_specs=[vmem],
        out_specs=vmem,
        scratch_shapes=[
            pltpu.VMEM((inner, samples, depth), jnp.bfloat16),
            pltpu.VMEM((slots,) + tag_shape, jnp.float32),
            pltpu.VMEM((slots, extra, LANES), jnp.int32),
            *[pltpu.SMEM((extra, LANES), jnp.int32)] * slots,
            pltpu.SemaphoreType.DMA((slots,)),
        ],
        cost_estimate=cost,
        compiler_params=small,
        name="tally_tail",
    )(arrived_tail)
    arrived = [sent[0]]
    for hop in range(1, inner):
        arrived.append(lax.ppermute(sent[hop], every, [(at, at ^ hop) for at in range(owners)]))
    rows = pl.pallas_call(
        functools.partial(tally_kernel, window, samples),
        out_shape=jax.ShapeDtypeStruct((owners, RQ + tail_rows, depth), jnp.bfloat16),
        in_specs=[vmem] * (1 + inner),
        out_specs=vmem,
        scratch_shapes=[
            pltpu.VMEM(tag_shape, jnp.float32),
            pltpu.VMEM((extra, LANES), jnp.int32),
            pltpu.SMEM((extra, LANES), jnp.int32),
            pltpu.SemaphoreType.DMA,
        ],
        cost_estimate=cost,
        compiler_params=small,
        name="tally",
    )(rows_tail, *arrived)
    table_grad = pl.pallas_call(
        functools.partial(finish_kernel, tail, keep, pieces),
        out_shape=jax.ShapeDtypeStruct((fields, RQ, depth), jnp.float32),
        in_specs=[vmem],
        out_specs=pl.BlockSpec(memory_space=pl.ANY),
        scratch_shapes=[pltpu.VMEM((fields, RQ, depth), jnp.float32), pltpu.SemaphoreType.DMA((fields,))],
        compiler_params=small,
        name="finish",
    )(exchange(rows, None).reshape(outer, inner, RQ + tail_rows, depth))
    return table_grad, dense_grad


def solution(mesh):
    tab, rep = mesh.shape["tab"], mesh.shape["rep"]
    inner = rep * math.gcd(tab, 4)
    every = ("tab", "rep")
    return jax.shard_map(
        functools.partial(local, tab * rep // inner, inner),
        mesh=mesh,
        in_specs=(P(every, None), P(every, None, None), P(None, every)),
        out_specs=(P(None, every, None), P(every, None)),
        check_vma=False,
    )
```

```python
import functools
import math

import jax
import jax.numpy as jnp
from jax import lax
from jax.experimental import pallas as pl
from jax.experimental.pallas import tpu as pltpu
from jax.sharding import PartitionSpec as P

RQ = 128
LANES = 128
PACK = 16
SUB = 8
HALVES = 2
PARTS = 8
GROUP = LANES // PARTS
GROUP_UNROLL = 32
OWNER_UNROLL = 32
EXACT = 256


def iota(shape, dim):
    return lax.broadcasted_iota(jnp.int32, shape, dim)


def one_hot(hit):
    return jnp.where(hit, 1.0, 0.0).astype(jnp.bfloat16)


def order_fields(first, count, owners, window, ids_ref, store, rank_ref, mine):
    samples = ids_ref.shape[1]
    pitch = LANES // HALVES
    last_tile = (samples - window) // PACK
    for at in range(count):
        own = ids_ref[first + at : first + at + 1, :] // RQ
        mine[at * owners : (at + 1) * owners, :] = one_hot(iota((owners, samples), 0) == own)
    earlier = one_hot(iota((samples, samples), 0) < iota((samples, samples), 1))
    before = jnp.dot(mine[...], earlier, preferred_element_type=jnp.float32)
    held = jnp.dot(mine[...], jnp.ones((samples, LANES), jnp.bfloat16), preferred_element_type=jnp.float32)
    below = one_hot(iota((owners, owners), 0) > iota((owners, owners), 1))
    slot_at = iota((LANES, samples), 0).astype(jnp.float32)
    lane = iota((owners // HALVES, LANES), 1)
    starts = [
        jnp.dot(below, held[at * owners : (at + 1) * owners].astype(jnp.bfloat16), preferred_element_type=jnp.float32)
        for at in range(count)
    ]
    placed = []
    for at, start in enumerate(starts):
        rows = slice(at * owners, (at + 1) * owners)
        tile = jnp.minimum(jnp.floor(start * (1.0 / PACK)), float(last_tile))
        hit = mine[rows, :].astype(jnp.float32)
        place = hit * (before[rows] + jnp.concatenate([start] * (samples // LANES), axis=1))
        base = hit * jnp.concatenate([tile * PACK] * (samples // LANES), axis=1)
        rank = jnp.sum(place, axis=0, keepdims=True)
        slot = rank - jnp.sum(base, axis=0, keepdims=True)
        rank_ref[at : at + 1, :] = rank
        placed.append((tile, slot))
    for at, (tile, slot) in enumerate(placed):
        hit = mine[at * owners : (at + 1) * owners, :].astype(jnp.float32)
        tag = (ids_ref[first + at : first + at + 1, :] % RQ + 1).astype(jnp.float32)
        tags = lax.dot_general(
            (hit * tag).astype(jnp.bfloat16),
            one_hot(slot_at == slot),
            (((1,), (1,)), ((), ())),
            preferred_element_type=jnp.float32,
        )
        half = owners // HALVES
        row = tags[:half] + pltpu.roll(tags[half:], pitch, 1)
        row = jnp.where(lane == pitch - 1, tile[:half], jnp.where(lane == LANES - 1, tile[half:], row))
        store(at, row.astype(jnp.bfloat16))


def lane_group(rows):
    return iota((rows, LANES), 1) // GROUP


def shift(block, groups):
    return pltpu.roll(block, groups * GROUP % LANES, 1) if groups % PARTS else block


def pick(block, first, count, other):
    group = lane_group(block.shape[0])
    return jnp.where((group >= first) & (group < first + count), block, other)


def fold(block, keep):
    rows = block.shape[0] // PARTS
    out = []
    for part in range(keep):
        kept = block[part * rows : (part + 1) * rows]
        for at in range(keep, PARTS):
            kept = pick(shift(block[at * rows : (at + 1) * rows], at - part), at, 1, kept)
        out.append(kept)
    return jnp.concatenate(out, axis=0)


def unfold(block, keep):
    rows = block.shape[0] // keep
    out = []
    for at in range(keep, PARTS):
        moved = jnp.zeros((rows, LANES), block.dtype)
        for part in range(keep):
            moved = pick(shift(block[part * rows : (part + 1) * rows], part - at), part, 1, moved)
        out.append(moved)
    return jnp.concatenate(out, axis=0)


def share_out(count, devices):
    keep = -(-count * PARTS // devices)
    rest, others = PARTS - keep, devices - count
    singles = keep - rest
    if singles < 0 or (count - others) * rest > others * singles:
        raise ValueError("unsupported sizes")
    pieces = [(at, 0, at, keep, 0, rest) for at in range(min(others, count))]
    for at in range(max(count - others, 0) * rest):
        slot = at % singles
        pieces.append((at // singles, 1 + slot, others + at // rest, keep + at % rest, rest + slot, 1))
    return keep, 1 + singles, pieces


def hop_order(devices):
    return sorted(range(devices), key=lambda hop: (hop > 0, -bin(hop).count("1")))


def send_kernel(first, count, tail, owners, window, me_ref, ids_hbm, pairs_hbm, feat_hbm, *rest):
    if tail:
        payload_hbm, *rest = rest
    else:
        dense_ref, *rest = rest
        payload_hbm, rest = rest[:count], rest[count:]
    ids_ref, pairs_ref, feat_ref, payload_ref, rank_ref, mine, weights, grads, in_done, out_done = rest
    inputs = [
        pltpu.make_async_copy(source, target, in_done.at[at])
        for at, (source, target) in enumerate([(ids_hbm, ids_ref), (pairs_hbm, pairs_ref), (feat_hbm, feat_ref)])
    ]
    for copy in inputs:
        copy.start()

    def leave(at, hop=0):
        target = payload_hbm.at[at] if tail else payload_hbm[hop]
        return pltpu.make_async_copy(payload_ref.at[at], target, out_done.at[at])

    vectors, samples, depth = feat_ref.shape
    span = 2 * LANES
    keep, slots, pieces = share_out(count, payload_ref.shape[0]) if tail else (PARTS, 1, [])
    body = samples * keep // PARTS
    extra = owners // HALVES
    for at in range(count, payload_ref.shape[0]):
        payload_ref[at, body:] = jnp.zeros((payload_ref.shape[1] - body, LANES), jnp.bfloat16)

    def store(at, row):
        homes = [(at, slot) for slot in range(slots)]
        homes += [(count + device, slot) for device, slot, field, *_ in pieces if field == at]
        for device, slot in homes:
            payload_ref[device, body + slot * extra : body + (slot + 1) * extra, :] = row

    inputs[0].wait()
    inputs[1].wait()
    order_fields(first, count, owners, window, ids_ref, store, rank_ref, mine)
    targets = ([] if tail else [0]) + list(range(first + 1, first + 1 + count))
    pairs = pairs_ref[...].astype(jnp.float32).T.astype(jnp.bfloat16)
    pair_at = iota((pairs.shape[1], span), 0)
    source = iota((1, span), 1) // SUB
    own_lane = one_hot(iota((PACK, span), 1) % SUB == iota((PACK, span), 0) % SUB)

    def spread_of(target):
        pair = jnp.where(source < target, target * (target - 1) // 2 + source, source * (source - 1) // 2 + target)
        pair = jnp.where((source == target) | (source >= vectors), -1, pair)
        found = jnp.dot(pairs, one_hot(pair_at == pair), preferred_element_type=jnp.float32)
        return found.reshape(samples // SUB, SUB, span)

    for at in range(0, len(targets), 2):
        low = spread_of(targets[at])
        high = spread_of(targets[at + 1]) if at + 1 < len(targets) else jnp.zeros_like(low)
        weights[:, at // 2] = jnp.concatenate([low, high], axis=1).astype(jnp.bfloat16) * own_lane
    inputs[2].wait()

    def per_group(group, carry):
        begin = pl.multiple_of(group * PACK, PACK)
        block = feat_ref[:, pl.ds(begin, PACK), :].astype(jnp.float32)
        outs = []
        for part in range(PACK // SUB):
            right = block[:, part * SUB : (part + 1) * SUB, :].reshape(vectors * SUB, depth)
            right = jnp.concatenate([right, jnp.zeros((span - vectors * SUB, depth), jnp.float32)], axis=0)
            left = weights[group * (PACK // SUB) + part].reshape(-1, span)
            out = jnp.dot(left, right.astype(jnp.bfloat16), preferred_element_type=jnp.float32)
            outs.append(out.reshape(-1, SUB, depth))
        out = jnp.concatenate(outs, axis=1)
        if not tail:
            dense_ref[pl.ds(begin, PACK), :] = out[0]
            out = out[1:]
        grads[:, pl.ds(begin, PACK), :] = out[:count].astype(jnp.bfloat16)
        return carry

    lax.fori_loop(0, samples // PACK, per_group, 0, unroll=GROUP_UNROLL)
    near = math.gcd(samples, EXACT)
    slot_at = iota((near, samples), 0).astype(jnp.float32).astype(jnp.bfloat16)

    def placed(at):
        rank = rank_ref[pl.ds(at, 1), :]
        tiles = []
        for top in range(0, samples, near):
            here = jnp.broadcast_to((rank - top).astype(jnp.bfloat16), (near, samples))
            tiles.append(jnp.where(slot_at == here, jnp.bfloat16(1), jnp.bfloat16(0)))
        placing = jnp.concatenate(tiles, axis=0)
        return jnp.dot(placing, grads[at], preferred_element_type=jnp.float32)

    if tail:
        for at in range(count):
            block = placed(at)
            grads[at] = block.astype(jnp.bfloat16)
            payload_ref[at, :body, :] = fold(block, keep).astype(jnp.bfloat16)
            leave(at).start()
        for at in range(payload_ref.shape[0] - count):
            block = jnp.zeros((samples, LANES), jnp.float32)
            for device, _, field, source, target, groups in pieces:
                if device == at:
                    block = pick(shift(grads[field].astype(jnp.float32), target - source), target, groups, block)
            payload_ref[count + at, :body, :] = fold(block, keep).astype(jnp.bfloat16)
            leave(count + at).start()
    else:

        def per_field(at, carry):
            payload_ref[at, :body, :] = placed(at).astype(jnp.bfloat16)
            for place, hop in enumerate(hop_order(count)):
                pl.when(lax.bitwise_xor(me_ref[0], at) == hop)(leave(at, place).start)
            return carry

        lax.fori_loop(0, count, per_field, 0, unroll=2)
    for at in range(payload_ref.shape[0]):
        leave(at).wait()


def read_tags(window, blocks, first_row, data_ref, tags, tiles):
    half, pitch = tiles.shape[0], LANES // HALVES
    lane = iota((half, LANES), 1)
    tags[...] = jnp.zeros_like(tags)
    found = jnp.zeros((half, LANES), jnp.float32)
    for block in range(blocks):
        rows = data_ref[block][first_row : first_row + half, :].astype(jnp.float32)
        column, offset = divmod(block * window, LANES)
        for part in range(HALVES):
            own = slice(part * half, (part + 1) * half)
            tile_lane = part * blocks + block
            found = jnp.where(
                lane == tile_lane, pltpu.roll(rows, (tile_lane - (part * pitch + pitch - 1)) % LANES, 1), found
            )
            shifted = pltpu.roll(rows, (offset - part * pitch) % LANES, 1) if offset != part * pitch else rows
            fits = min(window, LANES - offset)
            here = slice(column * LANES, (column + 1) * LANES)
            tags[own, here] = jnp.where((lane >= offset) & (lane < offset + fits), shifted, tags[own, here])
            if fits < window:
                after = slice((column + 1) * LANES, (column + 2) * LANES)
                tags[own, after] = jnp.where(lane < window - fits, shifted, tags[own, after])
    tiles[...] = found.astype(jnp.int32)


def rows_of(window, owner, sorted_ref, tags, tile_at):
    blocks = len(sorted_ref)
    half = tile_at.shape[0]
    part, row = owner // half, owner % half
    row_at = (iota((RQ, blocks * window), 0) + 1).astype(jnp.float32)
    picked = []
    for block in range(blocks):
        tile = tile_at[row, part * blocks + block]
        picked.append(sorted_ref[block][pl.ds(pl.multiple_of(tile * PACK, PACK), window), :])
    matches = one_hot(row_at == tags[pl.ds(owner, 1), : blocks * window])
    return jnp.dot(matches, jnp.concatenate(picked, axis=0), preferred_element_type=jnp.float32)


def tally_kernel(window, samples, tail_ref, *rest):
    *data_ref, out_ref, tags, tiles, tile_at, done = rest
    read_tags(window, len(data_ref), samples, data_ref, tags, tiles)
    copy = pltpu.make_async_copy(tiles, tile_at, done)
    copy.start()
    out_ref[:, RQ:, :] = tail_ref[...]
    copy.wait()

    def per_owner(owner, carry):
        out_ref[owner, :RQ, :] = rows_of(window, owner, data_ref, tags, tile_at).astype(jnp.bfloat16)
        return carry

    lax.fori_loop(0, out_ref.shape[0], per_owner, 0, unroll=OWNER_UNROLL)


def tally_tail_kernel(window, samples, keep, slots, data_ref, out_ref, unfolded, tags, tiles, *rest):
    blocks = data_ref.shape[0]
    half = tiles.shape[1]
    body = samples * keep // PARTS
    tile_at, done = rest[:slots], rest[slots]
    copies = []
    for slot in range(slots):
        read_tags(window, blocks, body + slot * half, [data_ref.at[at] for at in range(blocks)], tags.at[slot], tiles.at[slot])
        copies.append(pltpu.make_async_copy(tiles.at[slot], tile_at[slot], done.at[slot]))
        copies[-1].start()
    for block in range(blocks):
        unfolded[block, :body, :] = data_ref[block, :body, :]
        unfolded[block, body:, :] = unfold(data_ref[block, :body, :].astype(jnp.float32), keep).astype(jnp.bfloat16)
    for copy in copies:
        copy.wait()

    ordered = [unfolded.at[at] for at in range(blocks)]

    def per_owner(owner, carry):
        rows = rows_of(window, owner, ordered, tags.at[0], tile_at[0])
        for slot in range(1, slots):
            other = rows_of(window, owner, ordered, tags.at[slot], tile_at[slot])
            rows = pick(other, PARTS - keep + slot - 1, 1, rows)
        out_ref[owner] = fold(rows, keep).astype(jnp.bfloat16)
        return carry

    lax.fori_loop(0, out_ref.shape[0], per_owner, 0, unroll=2)


def finish_kernel(count, keep, pieces, data_ref, table_hbm, table_ref, done):
    inner = data_ref.shape[1]
    tails = []

    def leave(at):
        return pltpu.make_async_copy(table_ref.at[at], table_hbm.at[at], done.at[at])

    for at in range(inner):
        total = jnp.sum(data_ref[:, at].astype(jnp.float32), axis=0)
        table_ref[at] = total[:RQ]
        leave(at).start()
        tails.append(jnp.concatenate([total[RQ:], unfold(total[RQ:], keep)], axis=0))
    for at in range(count):
        rows = tails[at]
        for device, _, field, source, target, groups in pieces:
            if field == at:
                rows = pick(shift(tails[count + device], source - target), source, groups, rows)
        table_ref[inner + at] = rows
        leave(inner + at).start()
    for at in range(table_ref.shape[0]):
        leave(at).wait()


def local(outer, inner, sample_ids, features, pair_grad):
    samples, vectors, depth = features.shape
    fields = vectors - 1
    owners = outer * inner
    capacity = 2 * samples // owners
    window = min(-(-(PACK - 1 + capacity) // PACK) * PACK, samples)
    extra = owners // HALVES
    tail = fields - inner
    if depth != LANES or not 0 < tail <= inner:
        raise ValueError("unsupported sizes")
    keep, slots, pieces = share_out(tail, inner)
    every = ("tab", "rep")
    groups = [list(range(start, start + inner)) for start in range(0, owners, inner)]
    vmem = pl.BlockSpec(memory_space=pltpu.VMEM)
    params = pltpu.CompilerParams(vmem_limit_bytes=63 * 2**20)
    ids = sample_ids.T
    by_vector = features.transpose(1, 0, 2)
    me = jnp.reshape(lax.axis_index(every) % inner, (1,))
    tail_rows = RQ * keep // PARTS
    tag_shape = (owners, -(-inner * window // LANES) * LANES)

    def send(first, count, is_tail):
        targets = count + 1 - is_tail
        rows = samples * keep // PARTS + slots * extra if is_tail else samples + extra
        shapes = [jax.ShapeDtypeStruct((inner, rows, depth), jnp.bfloat16)]
        specs = [pl.BlockSpec(memory_space=pl.ANY)]
        if not is_tail:
            shapes = [jax.ShapeDtypeStruct((samples, depth), jnp.float32)]
            shapes += [jax.ShapeDtypeStruct((rows, depth), jnp.bfloat16)] * inner
            specs = [vmem] + specs * inner
        return pl.pallas_call(
            functools.partial(send_kernel, first, count, is_tail, owners, window),
            out_shape=shapes,
            in_specs=[pl.BlockSpec(memory_space=pltpu.SMEM)] + [pl.BlockSpec(memory_space=pl.ANY)] * 3,
            out_specs=specs,
            scratch_shapes=[
                pltpu.VMEM(ids.shape, ids.dtype),
                pltpu.VMEM(pair_grad.shape, pair_grad.dtype),
                pltpu.VMEM(by_vector.shape, by_vector.dtype),
                pltpu.VMEM((inner, rows, depth), jnp.bfloat16),
                pltpu.VMEM((count, samples), jnp.float32),
                pltpu.VMEM((count * owners, samples), jnp.bfloat16),
                pltpu.VMEM((samples // SUB, -(-targets // 2), PACK, 2 * LANES), jnp.bfloat16),
                pltpu.VMEM((count, samples, depth), jnp.bfloat16),
                pltpu.SemaphoreType.DMA((3,)),
                pltpu.SemaphoreType.DMA((inner,)),
            ],
            cost_estimate=pl.CostEstimate(
                flops=2 * targets * samples * samples * depth, bytes_accessed=2 * features.size, transcendentals=0
            ),
            compiler_params=params,
            name="send",
        )(me, ids, pair_grad, by_vector)

    def exchange(blocks, groups):
        return lax.all_to_all(blocks, every, split_axis=0, concat_axis=0, tiled=True, axis_index_groups=groups)

    small = pltpu.CompilerParams(vmem_limit_bytes=28 * 2**20)
    cost = pl.CostEstimate(
        flops=2 * owners * inner * window * RQ * depth, bytes_accessed=4 * inner * samples * depth, transcendentals=0
    )
    arrived_tail = exchange(send(inner, tail, True)[0], groups)
    dense_grad, *sent = send(0, inner, False)
    rows_tail = pl.pallas_call(
        functools.partial(tally_tail_kernel, window, samples, keep, slots),
        out_shape=jax.ShapeDtypeStruct((owners, tail_rows, depth), jnp.bfloat16),
        in_specs=[vmem],
        out_specs=vmem,
        scratch_shapes=[
            pltpu.VMEM((inner, samples, depth), jnp.bfloat16),
            pltpu.VMEM((slots,) + tag_shape, jnp.float32),
            pltpu.VMEM((slots, extra, LANES), jnp.int32),
            *[pltpu.SMEM((extra, LANES), jnp.int32)] * slots,
            pltpu.SemaphoreType.DMA((slots,)),
        ],
        cost_estimate=cost,
        compiler_params=small,
        name="tally_tail",
    )(arrived_tail)
    arrived = [sent[0]]
    for block, hop in zip(sent[1:], hop_order(inner)[1:]):
        arrived.append(lax.ppermute(block, every, [(at, at ^ hop) for at in range(owners)]))
    rows = pl.pallas_call(
        functools.partial(tally_kernel, window, samples),
        out_shape=jax.ShapeDtypeStruct((owners, RQ + tail_rows, depth), jnp.bfloat16),
        in_specs=[vmem] * (1 + inner),
        out_specs=vmem,
        scratch_shapes=[
            pltpu.VMEM(tag_shape, jnp.float32),
            pltpu.VMEM((extra, LANES), jnp.int32),
            pltpu.SMEM((extra, LANES), jnp.int32),
            pltpu.SemaphoreType.DMA,
        ],
        cost_estimate=cost,
        compiler_params=small,
        name="tally",
    )(rows_tail, *arrived)
    table_grad = pl.pallas_call(
        functools.partial(finish_kernel, tail, keep, pieces),
        out_shape=jax.ShapeDtypeStruct((fields, RQ, depth), jnp.float32),
        in_specs=[vmem],
        out_specs=pl.BlockSpec(memory_space=pl.ANY),
        scratch_shapes=[pltpu.VMEM((fields, RQ, depth), jnp.float32), pltpu.SemaphoreType.DMA((fields,))],
        compiler_params=small,
        name="finish",
    )(exchange(rows, None).reshape(outer, inner, RQ + tail_rows, depth))
    return table_grad, dense_grad


def solution(mesh):
    tab, rep = mesh.shape["tab"], mesh.shape["rep"]
    inner = rep * math.gcd(tab, 4)
    every = ("tab", "rep")
    return jax.shard_map(
        functools.partial(local, tab * rep // inner, inner),
        mesh=mesh,
        in_specs=(P(every, None), P(every, None, None), P(None, every)),
        out_specs=(P(None, every, None), P(every, None)),
        check_vma=False,
    )
```
